32 devices in a mesh: gx: 16 (over z, y, x), yz: 2 (over core).
Axes of the slice: x: 2, y: 2, z: 4, core: 2. Of those that a mesh axis runs over, the one named last changes fastest.
Arguments:
- magnet: bfloat16 [256, 3, 16, 256], P('yz', None, 'gx'), may hold values from -5 to 5
- newell: bfloat16 [256, 6, 16, 256], P('yz'), may hold values from -0.875 to 0.875
Outputs:
- field: bfloat16 [256, 3, 16, 256], P('yz', None, 'gx')
The draws below stay inside these ranges and needn't reach their ends.
All inputs are finite; a program needn't handle non-finite values.
Results may differ from the reference program's by a relative error of at most 0.0055.
Values may be sent and summed in bfloat16 or wider, within the bound.
A program may use at most 256 MiB of HBM per device.

```python
import math
import jax
import jax.numpy as jnp
from jax import lax

NY = 256
NZ = 256
NX = 16


def steps_of(key, extent, cuts, least, high):
    level, own = 1.0, jax.random.fold_in(key, 6)
    for position, parts in cuts:
        steps = jnp.exp(jax.random.uniform(jax.random.fold_in(own, position), (parts,), jnp.float32, least / len(cuts), high / len(cuts)))
        level = level * jnp.repeat(steps, extent[position] // parts).reshape([-1 if axis == position else 1 for axis in range(len(extent))])
    return level


def scatter_about(key, shape, scale, bound, pieces=(), held_as=jnp.bfloat16):
    level = steps_of(key, shape, pieces, -0.22, 0.18) if pieces else 1.0
    array = jax.random.normal(key, shape, jnp.float32) * scale * level
    return jnp.minimum(jnp.maximum(array, -bound), bound).astype(held_as)


def setup_inputs(seed: int = 0) -> dict:
    arg_keys = jax.random.split(jax.random.key(seed), 3)
    magnet = scatter_about(arg_keys[0], (NY, 3, NX, NZ), 1.0, 5.0, ((0, 2), (2, 16)))
    newell = scatter_about(arg_keys[1], (NY, 6, NX, NZ), (3 * NX) ** -0.5, 0.875, ((0, 2),))
    return {"magnet": magnet, "newell": newell}


EXCHANGE = 0.2


def dft_tables(row_count, col_count, length, row_first, col_first):
    row_ids = (row_first + jnp.arange(row_count, dtype=jnp.int32))[:, None]
    col_ids = (col_first + jnp.arange(col_count, dtype=jnp.int32))[None, :]
    angles = ((row_ids * col_ids) % length).astype(jnp.float32) * (2.0 * math.pi / length)
    return jnp.cos(angles).astype(jnp.bfloat16), jnp.sin(angles).astype(jnp.bfloat16)


def forward_y(z_rows, cos_y, sin_y):
    half_cols = z_rows.shape[-1] // 2
    cos_part = jnp.einsum("ky,ycxq->kcxq", cos_y.astype(jnp.float32), z_rows.astype(jnp.float32))
    sin_part = jnp.einsum("ky,ycxq->kcxq", sin_y.astype(jnp.float32), z_rows.astype(jnp.float32))
    return jnp.concatenate([cos_part[..., :half_cols] + sin_part[..., half_cols:], cos_part[..., half_cols:] - sin_part[..., :half_cols]], axis=-1)


def inverse_y(modes_in, cos_y, sin_y):
    half_cols = modes_in.shape[-1] // 2
    cos_part = jnp.einsum("yk,kcxq->ycxq", cos_y.astype(jnp.float32), modes_in.astype(jnp.float32))
    sin_part = jnp.einsum("yk,kcxq->ycxq", sin_y.astype(jnp.float32), modes_in.astype(jnp.float32))
    return jnp.concatenate([cos_part[..., :half_cols] - sin_part[..., half_cols:], cos_part[..., half_cols:] + sin_part[..., :half_cols]], axis=-1)


def convolve(kernel_rows, source, tgt_first, tgt_rows, src_first):
    src_rows = source.shape[2]
    half_cols = source.shape[3] // 2
    modes = source.shape[0]
    offset = (tgt_first + jnp.arange(tgt_rows, dtype=jnp.int32))[:, None] - (src_first + jnp.arange(src_rows, dtype=jnp.int32))[None, :]
    distance = jnp.abs(offset).astype(jnp.int32)
    sign_flip = jnp.where(offset >= 0, 1.0, -1.0).astype(jnp.float32)[None, :, :, None]
    picked = jnp.take(kernel_rows, distance.reshape(-1), axis=2).reshape(modes, 6, tgt_rows, src_rows, half_cols)

    def mix_term(kern_comp, source_comp, imag_part, signed):
        weight = picked[:, kern_comp].astype(jnp.float32)
        if signed:
            weight = weight * sign_flip
        if imag_part:
            values = source[:, source_comp, :, half_cols:]
        else:
            values = source[:, source_comp, :, :half_cols]
        return jnp.sum(weight * values.astype(jnp.float32)[:, None], axis=2)

    x_real = -(mix_term(0, 0, False, False) - mix_term(4, 1, True, True) - mix_term(5, 2, True, True))
    x_imag = -(mix_term(0, 0, True, False) + mix_term(4, 1, False, True) + mix_term(5, 2, False, True))
    y_real = -(-mix_term(4, 0, True, True) + mix_term(1, 1, False, False) + mix_term(3, 2, False, False))
    y_imag = -(mix_term(4, 0, False, True) + mix_term(1, 1, True, False) + mix_term(3, 2, True, False))
    z_real = -(-mix_term(5, 0, True, True) + mix_term(3, 1, False, False) + mix_term(2, 2, False, False))
    z_imag = -(mix_term(5, 0, False, True) + mix_term(3, 1, True, False) + mix_term(2, 2, True, False))
    return jnp.stack([jnp.concatenate([x_real, x_imag], axis=-1), jnp.concatenate([y_real, y_imag], axis=-1), jnp.concatenate([z_real, z_imag], axis=-1)], axis=1)


def block_conv(pairing):
    return convolve(pairing[0], pairing[1], 0, NX, 0)


def reference(magnet, newell):
    cos_z, sin_z = dft_tables(NZ, NZ, NZ, 0, 0)
    cos_y, sin_y = dft_tables(NY, NY, NY, 0, 0)
    forward_z = jnp.concatenate([cos_z, -sin_z], axis=1)
    z_rows = jnp.dot(magnet, forward_z, preferred_element_type=jnp.float32).astype(jnp.bfloat16)
    spectrum = forward_y(z_rows, cos_y, sin_y).astype(jnp.bfloat16)
    blocks = NY // 8
    spec_blocks = spectrum.reshape(blocks, 8, 3, NX, 2 * NZ)
    table_blocks = newell.reshape(blocks, 8, 6, NX, NZ)
    field_blocks = lax.map(block_conv, (table_blocks, spec_blocks))
    field_spec = field_blocks.reshape(NY, 3, NX, 2 * NZ).astype(jnp.bfloat16)
    g_rows = inverse_y(field_spec, cos_y, sin_y).astype(jnp.bfloat16)
    inverse_z = jnp.concatenate([cos_z, -sin_z], axis=0)
    demag_field = jnp.dot(g_rows, inverse_z, preferred_element_type=jnp.float32) / (NY * NZ)
    centre = magnet.astype(jnp.float32)
    step_x = centre[:, :, 1:] - centre[:, :, :-1]
    laplace = jnp.pad(step_x, ((0, 0), (0, 0), (0, 1), (0, 0))) - jnp.pad(step_x, ((0, 0), (0, 0), (1, 0), (0, 0)))
    laplace = laplace + jnp.roll(centre, 1, 0) + jnp.roll(centre, -1, 0) - 2.0 * centre
    laplace = laplace + jnp.roll(centre, 1, 3) + jnp.roll(centre, -1, 3) - 2.0 * centre
    return (demag_field + EXCHANGE * laplace).astype(jnp.bfloat16)
```

```python
import functools
import math

import jax
import jax.numpy as jnp
import ml_dtypes
import numpy as np
from jax import lax
from jax.experimental import pallas as pl
from jax.experimental.pallas import tpu as pltpu
from jax.sharding import PartitionSpec as P

EXCHANGE = 0.2
F32 = jnp.float32
BF16 = jnp.bfloat16
MESH = pl.DeviceIdType.MESH


def tables(couplers, parts, y_total, z_total):
    pairs = y_total // (couplers * parts * 2)
    rows = y_total // parts
    half_y = y_total // 2

    def trig(k, n, length):
        angle = (k[:, None] * n[None, :] % length) * (2.0 * math.pi / length)
        return np.cos(angle), np.sin(angle)

    def y_rows(part, n):
        blocks = []
        for m in range(couplers):
            t = (m * parts + part) * pairs + np.arange(pairs)
            cos, sin = trig(t, n, y_total)
            if t[0] == 0:
                sin[0] = trig(np.array([half_y]), n, y_total)[0][0]
            blocks += [cos, sin]
        return np.concatenate(blocks)

    half = z_total // 2
    cos, sin = trig(np.arange(z_total), np.arange(half), z_total)
    alternate = np.cos(math.pi * np.arange(z_total))
    z_fwd = np.concatenate([cos, -sin], axis=1)
    z_fwd[:, half] = alternate
    z_inv = -np.concatenate([cos, -sin], axis=1).T
    z_inv[0] = -0.5
    z_inv[half] = -0.5 * alternate
    reverse = np.zeros((z_total, half))
    for k in range(half):
        reverse[-k % z_total, k] = 1.0
    forward, inverse = [], []
    for part in range(parts):
        own_first = (np.arange(y_total) + part * rows) % y_total
        forward.append(y_rows(part, own_first))
        inverse.append(np.concatenate([y_rows(other, own_first[:rows]) for other in range(parts)]).T)
    cast = lambda a: np.asarray(a, np.float32).astype(ml_dtypes.bfloat16)
    return cast(np.stack(forward)), cast(np.stack(inverse)), cast(z_fwd), cast(z_inv), cast(reverse)


def kernel(
    groups, couplers, pairs, magnet, newell, y_fwd, y_inv, z_fwd, z_inv, rev, out,
    mag, nwl, yf, yi, zf, zi, rv, halo, zrow, spec, send, recv, kern, source, acc, back, fields, stack,
    lap, load_sem, swap_recv, pair_sem, halo_send, halo_recv, fwd_send, fwd_recv, bwd_send, bwd_recv,
    rel_sem, hand,
):
    g = lax.axis_index("gx")
    c = lax.axis_index("yz")
    other = 1 - c
    own = 2 * pairs
    rows = magnet.shape[1]
    cells = groups
    half = magnet.shape[2] // 2
    wide = 6 * half
    plane = math.gcd(couplers, 4)
    layers = groups // plane
    ring = couplers // 2
    first_q = (groups - couplers) // 2
    whole_tiles = own % 16 == 0

    coupler = jnp.logical_and(g >= first_q, g < first_q + couplers)
    m = jnp.clip(g - first_q, 0, couplers - 1)
    my_layer = g // plane
    low = 2 * my_layer < layers
    from_edge = jnp.where(low, my_layer, layers - 1 - my_layer)

    def layer_at(t):
        v = jnp.where(t <= from_edge, from_edge - t, t)
        return jnp.where(low, v, layers - 1 - v)

    def target(k):
        return layer_at(layers - 1 - k // plane) * plane + lax.rem(g + lax.rem(k, plane), plane)

    def forward_at(k):
        layer = k // plane
        layer = jnp.where(low, couplers // plane - 1 - layer, layer)
        return layer * plane + lax.rem(g + k % plane, plane)

    has_next, has_last = g < groups - 1, g > 0
    next_out = jnp.logical_and(has_next, jnp.logical_or(g + 1 < first_q, g + 1 >= first_q + couplers))
    last_out = jnp.logical_and(has_last, jnp.logical_or(g - 1 < first_q, g - 1 >= first_q + couplers))

    barrier = pltpu.get_barrier_semaphore()

    @pl.when(c == 0)
    def _():
        pl.semaphore_signal(barrier, inc=1, device_id=(g, 1), device_id_type=MESH)

    def greet(to):
        pl.semaphore_signal(barrier, inc=1, device_id=(to, 0), device_id_type=MESH)

    @pl.when(coupler)
    def _():
        for r in range(1, groups):
            greet(lax.rem(g + r, groups))

    @pl.when(jnp.logical_and(jnp.logical_not(coupler), has_next))
    def _():
        greet(g + 1)

    @pl.when(jnp.logical_and(jnp.logical_not(coupler), has_last))
    def _():
        greet(g - 1)

    loads = [
        pltpu.make_async_copy(magnet, mag.at[0], load_sem.at[0]),
        pltpu.make_async_copy(z_fwd, zf, load_sem.at[1]),
        pltpu.make_async_copy(y_fwd.at[c], yf, load_sem.at[2]),
    ]
    reverse = pltpu.make_async_copy(rev, rv, load_sem.at[3])
    late = [
        pltpu.make_async_copy(y_inv.at[c], yi, load_sem.at[4]),
        pltpu.make_async_copy(z_inv, zi, load_sem.at[5]),
    ]
    for copy in loads:
        copy.start()

    def newell_row(part, p):
        t = (2 * m + part) * pairs + p
        return (1 - c) * t + c * lax.rem(rows - t, rows)

    @pl.when(coupler)
    def _():
        for p in range(pairs):
            pltpu.make_async_copy(newell.at[newell_row(c, p)], nwl.at[c, p], load_sem.at[6]).start()
        reverse.start()

    for copy in late:
        copy.start()

    @pl.when(c == 1)
    def _():
        pl.semaphore_wait(barrier, 1)
        pl.semaphore_signal(hand.at[0], inc=1, device_id=(g, 0), device_id_type=MESH)

    @pl.when(c == 0)
    def _():
        pl.semaphore_wait(hand.at[0], 1)

    loads[0].wait()
    swap = [
        pltpu.make_async_remote_copy(
            src_ref=mag.at[0, comp],
            dst_ref=mag.at[1, comp],
            send_sem=pair_sem.at[0],
            recv_sem=swap_recv.at[comp],
            device_id=(g, other),
            device_id_type=MESH,
        )
        for comp in range(3)
    ]
    for copy in swap:
        copy.start()

    @pl.when(coupler)
    def _():
        for p in range(pairs):
            pltpu.make_async_remote_copy(
                src_ref=newell.at[newell_row(other, p)],
                dst_ref=nwl.at[c, p],
                send_sem=pair_sem.at[1],
                recv_sem=pair_sem.at[2],
                device_id=(g, other),
                device_id_type=MESH,
            ).start()

    far = pltpu.make_async_remote_copy(
        src_ref=nwl.at[c],
        dst_ref=nwl.at[other],
        send_sem=pair_sem.at[1],
        recv_sem=pair_sem.at[2],
        device_id=(g, other),
        device_id_type=MESH,
    )

    loads[1].wait()
    loads[2].wait()
    for side in range(2):
        for comp in range(3):
            if side == 1:
                swap[comp].wait_recv()
            zrow[pl.ds(side * rows, rows), pl.ds(2 * comp * half, 2 * half)] = jnp.dot(
                mag[side, comp], zf[...], preferred_element_type=F32
            ).astype(BF16)
            if side == 1:
                at = pl.ds(2 * comp * half, 2 * half)
                part = jnp.dot(yf[...], zrow[:, at], preferred_element_type=F32)
                if whole_tiles:
                    for i in range(couplers):
                        send[i, :, at] = part[i * own : (i + 1) * own].astype(BF16)
                else:
                    spec[:, at] = part
    if not whole_tiles:
        for i in range(couplers):
            send[i] = spec[pl.ds(i * own, own), :].astype(BF16)

    @pl.when(c == 0)
    def _():
        others = couplers - coupler.astype(jnp.int32) + next_out.astype(jnp.int32) + last_out.astype(jnp.int32)
        pl.semaphore_wait(barrier, 2 * others)
        pl.semaphore_signal(hand.at[1], inc=1, device_id=(g, 1), device_id_type=MESH)

    @pl.when(c == 1)
    def _():
        pl.semaphore_wait(hand.at[1], 1)

    def forward(to):
        return pltpu.make_async_remote_copy(
            src_ref=send.at[to],
            dst_ref=recv.at[g],
            send_sem=fwd_send.at[0],
            recv_sem=fwd_recv.at[my_layer],
            device_id=(first_q + to, c),
            device_id_type=MESH,
        )

    for k in range(couplers):
        @pl.when(first_q + forward_at(k) != g)
        def _():
            forward(forward_at(k)).start()

    def halo_copy(side):
        to = lax.rem(g + (1, groups - 1)[side], groups)
        return pltpu.make_async_remote_copy(
            src_ref=mag.at[0],
            dst_ref=halo.at[side],
            send_sem=halo_send.at[side],
            recv_sem=halo_recv.at[side],
            device_id=(to, c),
            device_id_type=MESH,
        )

    for side, inside in enumerate((has_next, has_last)):
        @pl.when(inside)
        def _():
            halo_copy(side).start()

    def waiter(ref, send_sem, recv_sem):
        return pltpu.make_async_remote_copy(
            src_ref=ref,
            dst_ref=ref,
            send_sem=send_sem,
            recv_sem=recv_sem,
            device_id=(g, other),
            device_id_type=MESH,
        )

    lane = lax.broadcasted_iota(jnp.int32, (pairs, half), 1)
    slot = lax.broadcasted_iota(jnp.int32, (pairs, half), 0)
    first_t = (2 * m + c) * pairs + slot
    al = first_t == 0
    ln = jnp.logical_and(lane == 0, first_t > 0)

    def wait_layer(layer):
        @pl.when(layer == my_layer)
        def _():
            waiter(recv.at[pl.ds(0, plane - 1)], fwd_send.at[0], fwd_recv.at[layer]).wait_recv()

        @pl.when(layer != my_layer)
        def _():
            waiter(recv.at[pl.ds(0, plane)], fwd_send.at[0], fwd_recv.at[layer]).wait_recv()

    def unpack(j):
        block = recv[j].astype(F32)
        for comp in range(3):
            re = block[:, 2 * comp * half : (2 * comp + 1) * half]
            im = block[:, (2 * comp + 1) * half : (2 * comp + 2) * half]
            cr, sr, ci, si = re[:pairs], re[pairs:], im[:pairs], im[pairs:]
            first_re = cr + jnp.where(jnp.logical_or(al, ln), 0.0, si)
            first_im = jnp.where(ln, 0.0, ci) - jnp.where(al, 0.0, sr)
            mirror_re = jnp.where(al, sr, jnp.where(ln, ci, cr - si))
            mirror_im = jnp.where(al, si, jnp.where(ln, -si, ci + sr))
            source[j, 2 * comp] = jnp.concatenate([first_re, mirror_re], axis=0)
            source[j, 2 * comp + 1] = jnp.concatenate([first_im, mirror_im], axis=0)

    def k_of(entry, d):
        start = pl.multiple_of((entry * cells + d) * own, own)
        return kern[pl.ds(start, own), :]

    def add_layer(layer, i):
        total = [acc[i, q] for q in range(6)]
        for p in range(plane):
            j = layer * plane + p
            d = jnp.abs(i - j)
            signed = jnp.where(i >= j, 4, 10)
            xx, yy, zz, yz = (k_of(e, d) for e in range(4))
            xy, xz = k_of(signed, d), k_of(signed + 1, d)
            xxi, yyi, zzi, yzi = (k_of(6 + e, d) for e in range(4))
            xr, xi, yr, yim, zr, zim = (source[j, q] for q in range(6))
            total[0] += xx * xr - xy * yim - xz * zim
            total[1] += xxi * xi + xy * yr + xz * zr
            total[2] += yy * yr + yz * zr - xy * xi
            total[3] += yyi * yim + yzi * zim + xy * xr
            total[4] += yz * yr + zz * zr - xz * xi
            total[5] += yzi * yim + zzi * zim + xz * xr
        return total

    def backward(i):
        return pltpu.make_async_remote_copy(
            src_ref=back.at[i],
            dst_ref=fields.at[c, m],
            send_sem=bwd_send.at[0],
            recv_sem=bwd_recv.at[m // ring],
            device_id=(i, c),
            device_id_type=MESH,
        )

    def prepare():
        recv[g] = send[m]
        for p in range(pairs):
            pltpu.make_async_copy(newell.at[newell_row(c, p)], nwl.at[c, p], load_sem.at[6]).wait()
        far.wait_recv()
        reverse.wait()
        table_rows = 6 * cells
        even_rows = 4 * cells
        lane0 = lax.broadcasted_iota(jnp.int32, (table_rows, half), 1) == 0
        even = lax.broadcasted_iota(jnp.int32, (table_rows, half), 0) < even_rows
        sign = jnp.where(even, 1.0, -1.0).astype(F32)
        for p in range(pairs):
            first = nwl[0, p].reshape(table_rows, 2 * half)
            mirror = nwl[1, p].reshape(table_rows, 2 * half)
            rev_first = jnp.dot(first, rv[...], preferred_element_type=F32)
            rev_mirror = jnp.dot(mirror, rv[...], preferred_element_type=F32)
            lo_first, hi_first = first[:, :half].astype(F32), first[:, half:].astype(F32)
            lo_mirror, hi_mirror = mirror[:, :half].astype(F32), mirror[:, half:].astype(F32)
            if p == 0:
                alone = ((2 * m + c) * pairs == 0).astype(F32)
                paired = 1.0 - alone
                of_first = alone * rev_first + paired * rev_mirror
                of_mirror = alone * rev_mirror + paired * rev_first
            else:
                of_first, of_mirror = rev_mirror, rev_first
            k_first = lo_first + sign * of_first
            k_mirror = lo_mirror + sign * of_mirror
            middle = hi_first + sign * hi_mirror
            if p == 0:
                i_first = jnp.where(lane0, alone * (2.0 * hi_first) + paired * k_first, k_first)
                i_mirror = jnp.where(lane0, alone * (2.0 * hi_mirror) + paired * middle, k_mirror)
                k_mirror = jnp.where(lane0, alone * k_mirror + paired * middle, k_mirror)
            else:
                k_mirror = jnp.where(lane0, middle, k_mirror)
                i_first, i_mirror = k_first, k_mirror
            for place, k_all, i_all in ((p, k_first, i_first), (pairs + p, k_mirror, i_mirror)):
                kern[pl.ds(place, table_rows, stride=own), :] = k_all
                kern[pl.ds(table_rows * own + place, even_rows, stride=own), :] = i_all[:even_rows]
                kern[pl.ds((table_rows + even_rows) * own + place, 2 * cells, stride=own), :] = -k_all[even_rows:]

    def couple():
        acc[...] = jnp.zeros(acc.shape, F32)

        def gather(t, carry):
            layer = layer_at(t)
            wait_layer(layer)
            for p in range(plane):
                unpack(layer * plane + p)

            def over(i, inner):
                total = add_layer(layer, i)
                for q in range(6):
                    acc[i, q] = total[q]
                return inner

            return lax.fori_loop(0, cells, over, carry)

        lax.fori_loop(0, layers - 1, gather, 0)
        layer = layer_at(layers - 1)
        wait_layer(layer)
        for p in range(plane):
            unpack(layer * plane + p)

        def finish(k, carry):
            i = target(k)
            total = add_layer(layer, i)
            for comp in range(3):
                re, im = total[2 * comp], total[2 * comp + 1]
                fr, mr, fi, mi = re[:pairs], re[pairs:], im[:pairs], im[pairs:]
                cos_re = fr + jnp.where(al, 0.0, jnp.where(ln, fr, mr))
                cos_im = jnp.where(ln, mr, fi) + jnp.where(al, 0.0, jnp.where(ln, mr, mi))
                sin_re = jnp.where(al, mr, jnp.where(ln, -fi, mi) - fi)
                sin_im = jnp.where(al, mi, jnp.where(ln, -mi, fr) - jnp.where(ln, mi, mr))
                back[i, :, pl.ds(2 * comp * half, half)] = jnp.concatenate([cos_re, sin_re], axis=0).astype(BF16)
                back[i, :, pl.ds((2 * comp + 1) * half, half)] = jnp.concatenate([cos_im, sin_im], axis=0).astype(BF16)
            before = target(jnp.maximum(k - 1, 0))

            @pl.when(jnp.logical_and(k > 0, before != g))
            def _():
                backward(before).start()

            return carry

        lax.fori_loop(0, cells, finish, 0)
        last = target(cells - 1)

        @pl.when(last != g)
        def _():
            backward(last).start()

        fields[c, m] = back[g]

    @pl.when(coupler)
    def _():
        prepare()

    for comp in range(3):
        full = jnp.concatenate([mag[0, comp], mag[1, comp]], axis=0).astype(F32)
        centre = full[:rows]
        total = pltpu.roll(full, 1, 0)[:rows] + pltpu.roll(full, 2 * rows - 1, 0)[:rows]
        total = total + pltpu.roll(centre, 1, 1) + pltpu.roll(centre, 2 * half - 1, 1)
        lap[comp] = total - 4.0 * centre

    @pl.when(coupler)
    def _():
        couple()

    for side, inside in enumerate((has_last, has_next)):
        @pl.when(inside)
        def _():
            halo_copy(side).wait_recv()

        @pl.when(jnp.logical_not(inside))
        def _():
            halo[side] = mag[0]

    for comp in range(3):
        centre = mag[0, comp].astype(F32)
        x_part = halo[0, comp].astype(F32) + halo[1, comp].astype(F32) - 2.0 * centre
        lap[comp] = EXCHANGE * (lap[comp] + x_part)

    def relay(n):
        return pltpu.make_async_remote_copy(
            src_ref=fields.at[c, pl.ds(n * ring, ring)],
            dst_ref=fields.at[c, pl.ds(n * ring, ring)],
            send_sem=rel_sem.at[0],
            recv_sem=rel_sem.at[1],
            device_id=(g, other),
            device_id_type=MESH,
        )

    rings = couplers // ring
    for k in range(rings):
        n = jnp.where(low, k, rings - 1 - k)
        mine = jnp.logical_and(coupler, m // ring == n)
        if ring > 1:
            @pl.when(mine)
            def _():
                waiter(fields.at[c, pl.ds(0, ring - 1)], bwd_send.at[0], bwd_recv.at[n]).wait_recv()

        @pl.when(jnp.logical_not(mine))
        def _():
            waiter(fields.at[c, pl.ds(0, ring)], bwd_send.at[0], bwd_recv.at[n]).wait_recv()

        relay(n).start()

    for copy in late:
        copy.wait()
    waiter(fields.at[other], rel_sem.at[0], rel_sem.at[1]).wait_recv()

    if whole_tiles:
        modes = fields[...].reshape(2 * couplers * own, wide)
    else:
        for part in range(2):
            for i in range(couplers):
                stack[pl.ds((part * couplers + i) * own, own), :] = fields[part, i].astype(F32)
        modes = stack[...].astype(BF16)
    scale = 1.0 / (2 * rows * 2 * half)
    for comp in range(3):
        at = slice(2 * comp * half, 2 * (comp + 1) * half)
        g_rows = jnp.dot(yi[...], modes[:, at], preferred_element_type=F32).astype(BF16)
        demag = jnp.dot(g_rows, zi[...], preferred_element_type=F32) * scale
        out[comp] = (demag + lap[comp]).astype(BF16)

    waiter(mag.at[0], pair_sem.at[0], pair_sem.at[2]).wait_send()
    waiter(fields.at[c], rel_sem.at[0], rel_sem.at[1]).wait_send()

    @pl.when(coupler)
    def _():
        far.wait_send()
        waiter(send.at[pl.ds(0, couplers - 1)], fwd_send.at[0], fwd_recv.at[0]).wait_send()
        waiter(back.at[pl.ds(0, groups - 1)], bwd_send.at[0], bwd_recv.at[0]).wait_send()

    @pl.when(jnp.logical_not(coupler))
    def _():
        waiter(send, fwd_send.at[0], fwd_recv.at[0]).wait_send()

    for side, inside in enumerate((has_next, has_last)):
        @pl.when(inside)
        def _():
            halo_copy(side).wait_send()


def on_device(magnet, newell, *consts):
    rows, _, x_cells, z_total = magnet.shape
    groups = lax.axis_size("gx")
    parts = lax.axis_size("yz")
    assert x_cells == 1 and parts == 2
    couplers = groups // 2
    y_total = rows * parts
    pairs = y_total // (couplers * parts * 2)
    own = 2 * pairs
    half = z_total // 2
    wide = 3 * z_total
    layers = groups // math.gcd(couplers, 4)
    any_ref = pl.BlockSpec(memory_space=pl.ANY)
    dma = pltpu.SemaphoreType.DMA
    planes = jnp.transpose(magnet[:, :, 0, :], (1, 0, 2))
    field = pl.pallas_call(
        functools.partial(kernel, groups, couplers, pairs),
        out_shape=pltpu.VMEM(planes.shape, BF16),
        in_specs=[any_ref] * 7,
        out_specs=pl.BlockSpec(memory_space=pltpu.VMEM),
        scratch_shapes=[
            pltpu.VMEM((2, 3, rows, z_total), BF16),
            pltpu.VMEM((2, pairs, 6, groups, z_total), BF16),
            pltpu.VMEM((rows, y_total), BF16),
            pltpu.VMEM((rows, y_total), BF16),
            pltpu.VMEM((z_total, z_total), BF16),
            pltpu.VMEM((z_total, z_total), BF16),
            pltpu.VMEM((z_total, half), BF16),
            pltpu.VMEM((2, 3, rows, z_total), BF16),
            pltpu.VMEM((y_total, wide), BF16),
            pltpu.VMEM((rows, wide), F32),
            pltpu.VMEM((couplers, own, wide), BF16),
            pltpu.VMEM((groups, own, wide), BF16),
            pltpu.VMEM((12 * groups * own, half), F32),
            pltpu.VMEM((groups, 6, own, half), F32),
            pltpu.VMEM((groups, 6, own, half), F32),
            pltpu.VMEM((groups, own, wide), BF16),
            pltpu.VMEM((2, couplers, own, wide), BF16),
            pltpu.VMEM((y_total, wide), F32),
            pltpu.VMEM((3, rows, z_total), F32),
            dma((7,)),
            dma((3,)),
            dma((3,)),
            dma((2,)),
            dma((2,)),
            dma((1,)),
            dma((layers,)),
            dma((1,)),
            dma((2,)),
            dma((2,)),
            pltpu.SemaphoreType.REGULAR((2,)),
        ],
        compiler_params=pltpu.CompilerParams(collective_id=0, has_side_effects=True),
    )(planes, newell, *consts)
    return jnp.transpose(field, (1, 0, 2))[:, :, None, :]


def solution(mesh):
    groups, parts = mesh.shape["gx"], mesh.shape["yz"]

    def run(magnet, newell):
        consts = tables(groups // 2, parts, magnet.shape[0], magnet.shape[3])
        body = lambda m, n: on_device(m, n, *[jnp.asarray(t) for t in consts])
        return jax.shard_map(
            body,
            mesh=mesh,
            in_specs=(P("yz", None, "gx", None), P("yz", None, None, None)),
            out_specs=P("yz", None, "gx", None),
            check_vma=False,
        )(magnet, newell)

    return run
```

```python
import functools
import math

import jax
import jax.numpy as jnp
import ml_dtypes
import numpy as np
from jax import lax
from jax.experimental import pallas as pl
from jax.experimental.pallas import tpu as pltpu
from jax.sharding import PartitionSpec as P

EXCHANGE = 0.2
F32 = jnp.float32
BF16 = jnp.bfloat16
MESH = pl.DeviceIdType.MESH


def tables(groups, parts, y_total, z_total):
    pairs = y_total // (groups * parts * 2)
    rows = y_total // parts
    half_y = y_total // 2

    def trig(k, n, length):
        angle = (k[:, None] * n[None, :] % length) * (2.0 * math.pi / length)
        return np.cos(angle), np.sin(angle)

    def y_rows(part, n):
        blocks = []
        for m in range(groups):
            t = (m * parts + part) * pairs + np.arange(pairs)
            cos, sin = trig(t, n, y_total)
            if t[0] == 0:
                sin[0] = trig(np.array([half_y]), n, y_total)[0][0]
            blocks += [cos, sin]
        return np.concatenate(blocks)

    half = z_total // 2
    cos, sin = trig(np.arange(z_total), np.arange(half), z_total)
    alternate = np.cos(math.pi * np.arange(z_total))
    z_fwd = np.concatenate([cos, -sin], axis=1)
    z_fwd[:, half] = alternate
    z_inv = -np.concatenate([cos, -sin], axis=1).T
    z_inv[0] = -0.5
    z_inv[half] = -0.5 * alternate
    reverse = np.zeros((z_total, half))
    for k in range(half):
        reverse[-k % z_total, k] = 1.0
    forward, inverse = [], []
    for part in range(parts):
        own_first = (np.arange(y_total) + part * rows) % y_total
        forward.append(y_rows(part, own_first))
        inverse.append(np.concatenate([y_rows(other, own_first[:rows]) for other in range(parts)]).T)
    cast = lambda a: np.asarray(a, np.float32).astype(ml_dtypes.bfloat16)
    return cast(np.stack(forward)), cast(np.stack(inverse)), cast(z_fwd), cast(z_inv), cast(reverse)


def kernel(
    groups, pairs, magnet, newell, y_fwd, y_inv, z_fwd, z_inv, rev, out,
    mag, nwl, yf, yi, zf, zi, rv, zrow, spec, send, recv, kern, acc, back, fields, stack,
    lap, load_sem, swap_recv, pair_sem, fwd_send, fwd_recv, bwd_send, bwd_recv,
    rel_sem, hand,
):
    g = lax.axis_index("gx")
    c = lax.axis_index("yz")
    other = 1 - c
    own = 2 * pairs
    rows = magnet.shape[1]
    cells = groups
    half = magnet.shape[2] // 2
    wide = 6 * half
    plane = math.gcd(groups, 4)
    layers = groups // plane
    whole_tiles = own % 8 == 0

    last = groups - 1
    extra = groups // 4 + 1
    active = (g != last, g == extra)
    blocks = (g, last)

    def owner(b):
        return jnp.where(b == last, extra, b)

    my_layer = g // plane
    low = 2 * my_layer < layers
    from_edge = jnp.where(low, my_layer, layers - 1 - my_layer)

    def layer_at(t):
        v = jnp.where(t <= from_edge, from_edge - t, t)
        return jnp.where(low, v, layers - 1 - v)

    def target(k):
        return layer_at(layers - 1 - k // plane) * plane + lax.rem(g + lax.rem(k, plane), plane)

    barrier = pltpu.get_barrier_semaphore()

    @pl.when(c == 0)
    def _():
        pl.semaphore_signal(barrier, inc=1, device_id=(g, 1), device_id_type=MESH)

    def greet(to):
        pl.semaphore_signal(barrier, inc=1, device_id=(to, 0), device_id_type=MESH)

    @pl.when(g != last)
    def _():
        for r in range(1, groups):
            greet(lax.rem(g + r, groups))

    loads = [
        pltpu.make_async_copy(magnet, mag.at[0], load_sem.at[0]),
        pltpu.make_async_copy(z_fwd, zf, load_sem.at[1]),
        pltpu.make_async_copy(y_fwd.at[c], yf, load_sem.at[2]),
    ]
    reverse = pltpu.make_async_copy(rev, rv, load_sem.at[3])
    late = [
        pltpu.make_async_copy(y_inv.at[c], yi, load_sem.at[4]),
        pltpu.make_async_copy(z_inv, zi, load_sem.at[5]),
    ]
    for copy in loads:
        copy.start()

    def newell_row(slot, part, p):
        t = (2 * blocks[slot] + part) * pairs + p
        return (1 - c) * t + c * lax.rem(rows - t, rows)

    def near(slot, p):
        at = slot * pairs + p
        return pltpu.make_async_copy(newell.at[newell_row(slot, c, p)], nwl.at[c, at], load_sem.at[6 + slot])

    for slot in range(2):
        @pl.when(active[slot])
        def _():
            for p in range(pairs):
                near(slot, p).start()

    @pl.when(g != last)
    def _():
        reverse.start()

    for copy in late:
        copy.start()

    @pl.when(c == 1)
    def _():
        pl.semaphore_wait(barrier, 1)
        pl.semaphore_signal(hand.at[0], inc=1, device_id=(g, 0), device_id_type=MESH)

    @pl.when(c == 0)
    def _():
        pl.semaphore_wait(hand.at[0], 1)

    loads[0].wait()
    swap = [
        pltpu.make_async_remote_copy(
            src_ref=mag.at[0, comp],
            dst_ref=mag.at[1, comp],
            send_sem=pair_sem.at[0],
            recv_sem=swap_recv.at[comp],
            device_id=(g, other),
            device_id_type=MESH,
        )
        for comp in range(3)
    ]
    for copy in swap:
        copy.start()

    def far(slot, p, count):
        at = pl.ds(slot * pairs + p, count)
        row = newell_row(slot, other, p)
        return pltpu.make_async_remote_copy(
            src_ref=newell.at[pl.ds(row, 1)] if count == 1 else nwl.at[c, at],
            dst_ref=nwl.at[c, at],
            send_sem=pair_sem.at[1 + slot],
            recv_sem=pair_sem.at[3 + slot],
            device_id=(g, other),
            device_id_type=MESH,
        )

    for slot in range(2):
        @pl.when(active[slot])
        def _():
            for p in range(pairs):
                far(slot, p, 1).start()

    loads[1].wait()
    loads[2].wait()
    for side in range(2):
        for comp in range(3):
            if side == 1:
                swap[comp].wait_recv()
            zrow[pl.ds(side * rows, rows), pl.ds(2 * comp * half, 2 * half)] = jnp.dot(
                mag[side, comp], zf[...], preferred_element_type=F32
            ).astype(BF16)
            if side == 1:
                at = pl.ds(2 * comp * half, 2 * half)
                part = jnp.dot(yf[...], zrow[:, at], preferred_element_type=F32)
                if whole_tiles:
                    for i in range(groups):
                        send[i, :, at] = part[i * own : (i + 1) * own].astype(BF16)
                else:
                    spec[:, at] = part
    if not whole_tiles:
        for i in range(groups):
            send[i] = spec[pl.ds(i * own, own), :].astype(BF16)

    @pl.when(c == 0)
    def _():
        pl.semaphore_wait(barrier, 2 * (last - (g != last).astype(jnp.int32)))
        pl.semaphore_signal(hand.at[1], inc=1, device_id=(g, 1), device_id_type=MESH)

    @pl.when(c == 1)
    def _():
        pl.semaphore_wait(hand.at[1], 1)

    def forward(b):
        slot = (b == last).astype(jnp.int32)
        return pltpu.make_async_remote_copy(
            src_ref=send.at[b],
            dst_ref=recv.at[slot, g],
            send_sem=fwd_send.at[0],
            recv_sem=fwd_recv.at[slot * layers + my_layer],
            device_id=(owner(b), c),
            device_id_type=MESH,
        )

    for k in range(groups):
        b = target(k)

        @pl.when(owner(b) != g)
        def _():
            forward(b).start()

    def waiter(ref, send_sem, recv_sem):
        return pltpu.make_async_remote_copy(
            src_ref=ref,
            dst_ref=ref,
            send_sem=send_sem,
            recv_sem=recv_sem,
            device_id=(g, other),
            device_id_type=MESH,
        )

    lane = lax.broadcasted_iota(jnp.int32, (own, half), 1)
    row = lax.broadcasted_iota(jnp.int32, (own, half), 0)
    top = row < pairs

    def masks(slot):
        first_t = (2 * blocks[slot] + c) * pairs + lax.rem(row, pairs)
        al = first_t == 0
        ln = jnp.logical_and(lane == 0, first_t > 0)
        return al, jnp.logical_or(al, ln), jnp.logical_and(ln, jnp.logical_not(top))

    def flip(v):
        return jnp.concatenate([v[pairs:], v[:pairs]], axis=0)

    def wait_layer(slot, layer):
        sem = fwd_recv.at[slot * layers + layer]

        @pl.when(layer == my_layer)
        def _():
            waiter(recv.at[slot, pl.ds(0, plane - 1)], fwd_send.at[0], sem).wait_recv()

        @pl.when(layer != my_layer)
        def _():
            waiter(recv.at[slot, pl.ds(0, plane)], fwd_send.at[0], sem).wait_recv()

    def unpack(slot, j):
        al, special, ln_low = masks(slot)
        block = recv[slot, j].astype(F32)
        parts = []
        for comp in range(3):
            re = block[:, 2 * comp * half : (2 * comp + 1) * half]
            im = block[:, (2 * comp + 1) * half : (2 * comp + 2) * half]
            re_f, im_f = flip(re), flip(im)
            new_re = jnp.where(top, re + im_f, re_f - im)
            new_im = jnp.where(top, im - re_f, im_f + re)
            lone_re = jnp.where(ln_low, im_f, re)
            lone_im = jnp.where(al, im, -jnp.where(top, re_f, im))
            parts.append(jnp.where(special, lone_re, new_re))
            parts.append(jnp.where(special, lone_im, new_im))
        return parts

    def k_of(slot, entry, d):
        start = pl.multiple_of(((slot * 12 + entry) * cells + d) * own, own)
        return kern[pl.ds(start, own), :]

    def add_layer(slot, layer, sources, i):
        total = [acc[slot, i, q] for q in range(6)]
        for p in range(plane):
            j = layer * plane + p
            d = jnp.abs(i - j)
            signed = jnp.where(i >= j, 4, 10)
            xx, yy, zz, yz = (k_of(slot, e, d) for e in range(4))
            xy, xz = k_of(slot, signed, d), k_of(slot, signed + 1, d)
            xxi, yyi, zzi, yzi = (k_of(slot, 6 + e, d) for e in range(4))
            xr, xi, yr, yim, zr, zim = sources[p]
            total[0] += xx * xr - xy * yim - xz * zim
            total[1] += xxi * xi + xy * yr + xz * zr
            total[2] += yy * yr + yz * zr - xy * xi
            total[3] += yyi * yim + yzi * zim + xy * xr
            total[4] += yz * yr + zz * zr - xz * xi
            total[5] += yzi * yim + zzi * zim + xz * xr
        return total

    def backward(slot, i):
        return pltpu.make_async_remote_copy(
            src_ref=back.at[slot, i],
            dst_ref=fields.at[c, blocks[slot]],
            send_sem=bwd_send.at[0],
            recv_sem=bwd_recv.at[blocks[slot] // plane],
            device_id=(i, c),
            device_id_type=MESH,
        )

    def prepare(slot):
        recv[slot, g] = send[blocks[slot]]
        for p in range(pairs):
            near(slot, p).wait()
        far(slot, 0, pairs).wait_recv()
        table_rows = 6 * cells
        even_rows = 4 * cells
        lane0 = lax.broadcasted_iota(jnp.int32, (table_rows, half), 1) == 0
        even = lax.broadcasted_iota(jnp.int32, (table_rows, half), 0) < even_rows
        sign = jnp.where(even, 1.0, -1.0).astype(F32)
        row_of = lax.broadcasted_iota(jnp.int32, (table_rows, half), 0)
        diagonal = functools.reduce(jnp.logical_or, [row_of == entry * cells + 1 for entry in range(3)])
        neighbour = jnp.where(diagonal, -2.0 * EXCHANGE, 0.0).astype(F32)
        base = slot * 12 * cells * own
        for p in range(pairs):
            first = nwl[0, slot * pairs + p].reshape(table_rows, 2 * half)
            mirror = nwl[1, slot * pairs + p].reshape(table_rows, 2 * half)
            rev_first = jnp.dot(first, rv[...], preferred_element_type=F32)
            rev_mirror = jnp.dot(mirror, rv[...], preferred_element_type=F32)
            lo_first, hi_first = first[:, :half].astype(F32), first[:, half:].astype(F32)
            lo_mirror, hi_mirror = mirror[:, :half].astype(F32), mirror[:, half:].astype(F32)
            if p == 0:
                alone = ((2 * blocks[slot] + c) * pairs == 0).astype(F32)
                paired = 1.0 - alone
                of_first = alone * rev_first + paired * rev_mirror
                of_mirror = alone * rev_mirror + paired * rev_first
            else:
                of_first, of_mirror = rev_mirror, rev_first
            k_first = lo_first + sign * of_first
            k_mirror = lo_mirror + sign * of_mirror
            middle = hi_first + sign * hi_mirror
            if p == 0:
                i_first = jnp.where(lane0, alone * (2.0 * hi_first) + paired * k_first, k_first)
                i_mirror = jnp.where(lane0, alone * (2.0 * hi_mirror) + paired * middle, k_mirror)
                k_mirror = jnp.where(lane0, alone * k_mirror + paired * middle, k_mirror)
            else:
                k_mirror = jnp.where(lane0, middle, k_mirror)
                i_first, i_mirror = k_first, k_mirror
            for place, k_all, i_all in ((p, k_first, i_first), (pairs + p, k_mirror, i_mirror)):
                k_all, i_all = k_all + neighbour, i_all + neighbour
                kern[pl.ds(base + place, table_rows, stride=own), :] = k_all
                kern[pl.ds(base + table_rows * own + place, even_rows, stride=own), :] = i_all[:even_rows]
                kern[pl.ds(base + (table_rows + even_rows) * own + place, 2 * cells, stride=own), :] = -k_all[even_rows:]
        acc[slot] = jnp.zeros(acc.shape[1:], F32)

    def gather(slot, layer):
        wait_layer(slot, layer)
        sources = [unpack(slot, layer * plane + p) for p in range(plane)]

        def over(n, inner):
            for p in range(plane):
                i = n * plane + p
                total = add_layer(slot, layer, sources, i)
                for q in range(6):
                    acc[slot, i, q] = total[q]
            return inner

        lax.fori_loop(0, layers, over, 0)

    def finish(slot, layer):
        wait_layer(slot, layer)
        sources = [unpack(slot, layer * plane + p) for p in range(plane)]
        al, special, _ = masks(slot)

        def dispatch(n):
            for p in range(plane):
                i = target(n * plane + p)

                @pl.when(i != g)
                def _():
                    backward(slot, i).start()

        def over(n, carry):
            for p in range(plane):
                i = target(n * plane + p)
                spread(i, add_layer(slot, layer, sources, i))

            @pl.when(n > 0)
            def _():
                dispatch(jnp.maximum(n - 1, 0))

            return carry

        def spread(i, total):
            for comp in range(3):
                re, im = total[2 * comp], total[2 * comp + 1]
                re_f, im_f = flip(re), flip(im)
                new_re = jnp.where(top, re + re_f, im - im_f)
                new_im = jnp.where(top, im + im_f, re_f - re)
                lone_re = jnp.where(al, re, 2.0 * jnp.where(top, re, -im_f))
                lone_im = jnp.where(al, im, 2.0 * jnp.where(top, re_f, -im))
                new_re = jnp.where(special, lone_re, new_re)
                new_im = jnp.where(special, lone_im, new_im)
                back[slot, i, :, pl.ds(2 * comp * half, half)] = new_re.astype(BF16)
                back[slot, i, :, pl.ds((2 * comp + 1) * half, half)] = new_im.astype(BF16)

        lax.fori_loop(0, layers, over, 0)
        dispatch(layers - 1)
        fields[c, blocks[slot]] = back[slot, g]

    @pl.when(g != last)
    def _():
        reverse.wait()

    for slot in range(2):
        @pl.when(active[slot])
        def _():
            prepare(slot)

    beside = (g > 0).astype(F32) + (g < groups - 1).astype(F32)
    for comp in range(3):
        full = jnp.concatenate([mag[0, comp], mag[1, comp]], axis=0).astype(F32)
        centre = full[:rows]
        total = pltpu.roll(full, 1, 0)[:rows] + pltpu.roll(full, 2 * rows - 1, 0)[:rows]
        total = total + pltpu.roll(centre, 1, 1) + pltpu.roll(centre, 2 * half - 1, 1)
        lap[comp] = EXCHANGE * (total - (4.0 + beside) * centre)

    def step(t, carry):
        for slot in range(2):
            @pl.when(active[slot])
            def _():
                gather(slot, layer_at(t))
        return carry

    lax.fori_loop(0, layers - 1, step, 0)
    for slot in range(2):
        @pl.when(active[slot])
        def _():
            finish(slot, layer_at(layers - 1))

    def relay(n):
        return pltpu.make_async_remote_copy(
            src_ref=fields.at[c, pl.ds(n * plane, plane)],
            dst_ref=fields.at[c, pl.ds(n * plane, plane)],
            send_sem=rel_sem.at[0],
            recv_sem=rel_sem.at[1],
            device_id=(g, other),
            device_id_type=MESH,
        )

    for k in range(layers):
        n = layer_at(k)
        mine = jnp.logical_and(g != last, n == my_layer)
        local = mine.astype(jnp.int32) + jnp.logical_and(g == extra, n == last // plane).astype(jnp.int32)
        for count in range(plane - 2, plane + 1):
            if count > 0:
                @pl.when(plane - local == count)
                def _():
                    waiter(fields.at[c, pl.ds(0, count)], bwd_send.at[0], bwd_recv.at[n]).wait_recv()

        relay(n).start()

    for copy in late:
        copy.wait()
    waiter(fields.at[other], rel_sem.at[0], rel_sem.at[1]).wait_recv()

    if whole_tiles:
        modes = fields[...].reshape(2 * groups * own, wide)
    else:
        for part in range(2):
            for i in range(groups):
                stack[pl.ds((part * groups + i) * own, own), :] = fields[part, i].astype(F32)
        modes = stack[...].astype(BF16)
    scale = 1.0 / (2 * rows * 2 * half)
    for comp in range(3):
        at = slice(2 * comp * half, 2 * (comp + 1) * half)
        g_rows = jnp.dot(yi[...], modes[:, at], preferred_element_type=F32).astype(BF16)
        demag = jnp.dot(g_rows, zi[...], preferred_element_type=F32) * scale
        out[comp] = (demag + lap[comp]).astype(BF16)

    waiter(mag.at[0], pair_sem.at[0], swap_recv.at[0]).wait_send()
    waiter(fields.at[c], rel_sem.at[0], rel_sem.at[1]).wait_send()
    for slot in range(2):
        @pl.when(active[slot])
        def _():
            far(slot, 0, pairs).wait_send()
            waiter(back.at[slot, pl.ds(0, groups - 1)], bwd_send.at[0], bwd_recv.at[0]).wait_send()

    kept = active[0].astype(jnp.int32) + active[1].astype(jnp.int32)
    for count in range(3):
        @pl.when(kept == count)
        def _():
            waiter(send.at[pl.ds(0, groups - count)], fwd_send.at[0], fwd_recv.at[0]).wait_send()


def on_device(magnet, newell, *consts):
    rows, _, x_cells, z_total = magnet.shape
    groups = lax.axis_size("gx")
    parts = lax.axis_size("yz")
    assert x_cells == 1 and parts == 2
    y_total = rows * parts
    pairs = y_total // (groups * parts * 2)
    own = 2 * pairs
    half = z_total // 2
    wide = 3 * z_total
    layers = groups // math.gcd(groups, 4)
    any_ref = pl.BlockSpec(memory_space=pl.ANY)
    dma = pltpu.SemaphoreType.DMA
    planes = jnp.transpose(magnet[:, :, 0, :], (1, 0, 2))
    field = pl.pallas_call(
        functools.partial(kernel, groups, pairs),
        out_shape=pltpu.VMEM(planes.shape, BF16),
        in_specs=[any_ref] * 7,
        out_specs=pl.BlockSpec(memory_space=pltpu.VMEM),
        scratch_shapes=[
            pltpu.VMEM((2, 3, rows, z_total), BF16),
            pltpu.VMEM((2, 2 * pairs, 6, groups, z_total), BF16),
            pltpu.VMEM((rows, y_total), BF16),
            pltpu.VMEM((rows, y_total), BF16),
            pltpu.VMEM((z_total, z_total), BF16),
            pltpu.VMEM((z_total, z_total), BF16),
            pltpu.VMEM((z_total, half), BF16),
            pltpu.VMEM((y_total, wide), BF16),
            pltpu.VMEM((rows, wide), F32),
            pltpu.VMEM((groups, own, wide), BF16),
            pltpu.VMEM((2, groups, own, wide), BF16),
            pltpu.VMEM((2 * 12 * groups * own, half), F32),
            pltpu.VMEM((2, groups, 6, own, half), F32),
            pltpu.VMEM((2, groups, own, wide), BF16),
            pltpu.VMEM((2, groups, own, wide), BF16),
            pltpu.VMEM((y_total, wide), F32),
            pltpu.VMEM((3, rows, z_total), F32),
            dma((8,)),
            dma((3,)),
            dma((5,)),
            dma((1,)),
            dma((2 * layers,)),
            dma((1,)),
            dma((layers,)),
            dma((2,)),
            pltpu.SemaphoreType.REGULAR((2,)),
        ],
        compiler_params=pltpu.CompilerParams(collective_id=0, has_side_effects=True),
    )(planes, newell, *consts)
    return jnp.transpose(field, (1, 0, 2))[:, :, None, :]


def solution(mesh):
    groups, parts = mesh.shape["gx"], mesh.shape["yz"]

    def run(magnet, newell):
        consts = tables(groups, parts, magnet.shape[0], magnet.shape[3])
        body = lambda m, n: on_device(m, n, *[jnp.asarray(t) for t in consts])
        return jax.shard_map(
            body,
            mesh=mesh,
            in_specs=(P("yz", None, "gx", None), P("yz", None, None, None)),
            out_specs=P("yz", None, "gx", None),
            check_vma=False,
        )(magnet, newell)

    return run
```

```python
import functools
import math

import jax
import jax.numpy as jnp
import ml_dtypes
import numpy as np
from jax import lax
from jax.experimental import pallas as pl
from jax.experimental.pallas import tpu as pltpu
from jax.sharding import PartitionSpec as P

EXCHANGE = 0.2
F32 = jnp.float32
BF16 = jnp.bfloat16
MESH = pl.DeviceIdType.MESH


def tables(groups, parts, y_total, z_total):
    pairs = y_total // (groups * parts * 2)
    rows = y_total // parts
    half_y = y_total // 2

    def trig(k, n, length):
        angle = (k[:, None] * n[None, :] % length) * (2.0 * math.pi / length)
        return np.cos(angle), np.sin(angle)

    def y_rows(part, n):
        blocks = []
        for m in range(groups):
            t = (m * parts + part) * pairs + np.arange(pairs)
            cos, sin = trig(t, n, y_total)
            if t[0] == 0:
                sin[0] = trig(np.array([half_y]), n, y_total)[0][0]
            blocks += [cos, sin]
        return np.concatenate(blocks)

    half = z_total // 2
    cos, sin = trig(np.arange(z_total), np.arange(half), z_total)
    alternate = np.cos(math.pi * np.arange(z_total))
    z_fwd = np.concatenate([cos, -sin], axis=1)
    z_fwd[:, half] = alternate
    z_inv = -np.concatenate([cos, -sin], axis=1).T
    z_inv[0] = -0.5
    z_inv[half] = -0.5 * alternate
    reverse = np.zeros((z_total, half))
    for k in range(half):
        reverse[-k % z_total, k] = 1.0
    forward, inverse = [], []
    for part in range(parts):
        own_first = (np.arange(y_total) + part * rows) % y_total
        forward.append(y_rows(part, own_first))
        inverse.append(np.concatenate([y_rows(other, own_first[:rows]) for other in range(parts)]).T)
    cast = lambda a: np.asarray(a, np.float32).astype(ml_dtypes.bfloat16)
    return cast(np.stack(forward)), cast(np.stack(inverse)), cast(z_fwd), cast(z_inv), cast(reverse)


def kernel(
    groups, pairs, magnet, newell, y_fwd, y_inv, z_fwd, z_inv, rev, out,
    mag, nwl, yf, yi, zf, zi, rv, zrow, spec, send, recv, kern, acc, back, fields, stack,
    lap, load_sem, near_sem, swap_recv, pair_sem, fwd_send, fwd_recv, bwd_send, bwd_recv,
    rel_sem, hand,
):
    g = lax.axis_index("gx")
    c = lax.axis_index("yz")
    other = 1 - c
    own = 2 * pairs
    rows = magnet.shape[1]
    cells = groups
    half = magnet.shape[2] // 2
    wide = 6 * half
    plane = math.gcd(groups, 4)
    layers = groups // plane
    whole_tiles = own % 8 == 0

    my_layer = g // plane
    low = 2 * my_layer < layers
    from_edge = jnp.where(low, my_layer, layers - 1 - my_layer)

    def layer_at(t):
        v = jnp.where(t <= from_edge, from_edge - t, t)
        return jnp.where(low, v, layers - 1 - v)

    def target(k):
        return lax.rem(g + k, groups)

    def relay_at(t):
        return layer_at(t)

    def group_at(t):
        return lax.rem(my_layer + layers - t, layers)

    barrier = pltpu.get_barrier_semaphore()
    loads = [
        pltpu.make_async_copy(magnet.at[comp], mag.at[0, comp], load_sem.at[comp]) for comp in range(3)
    ]
    tabs = [
        pltpu.make_async_copy(z_fwd, zf, load_sem.at[3]),
        pltpu.make_async_copy(y_fwd.at[c], yf, load_sem.at[4]),
    ]
    late = [
        pltpu.make_async_copy(rev, rv, load_sem.at[5]),
        pltpu.make_async_copy(y_inv.at[c], yi, load_sem.at[6]),
        pltpu.make_async_copy(z_inv, zi, load_sem.at[7]),
    ]
    for copy in loads:
        copy.start()

    @pl.when(c == 0)
    def _():
        pl.semaphore_signal(barrier, inc=1, device_id=(g, 1), device_id_type=MESH)

    for copy in tabs:
        copy.start()
    for r in range(1, groups):
        pl.semaphore_signal(barrier, inc=1, device_id=(lax.rem(g + r, groups), 0), device_id_type=MESH)

    def newell_row(part, p):
        t = (2 * g + part) * pairs + p
        return (1 - c) * t + c * lax.rem(rows - t, rows)

    near = [
        pltpu.make_async_copy(newell.at[newell_row(c, p)], nwl.at[c, p], near_sem.at[0]) for p in range(pairs)
    ]

    @pl.when(c == 1)
    def _():
        pl.semaphore_wait(barrier, 1)
        pl.semaphore_signal(hand.at[0], inc=1, device_id=(g, 0), device_id_type=MESH)

    @pl.when(c == 0)
    def _():
        pl.semaphore_wait(hand.at[0], 1)

    swap = [
        pltpu.make_async_remote_copy(
            src_ref=mag.at[0, comp],
            dst_ref=mag.at[1, comp],
            send_sem=pair_sem.at[0],
            recv_sem=swap_recv.at[comp],
            device_id=(g, other),
            device_id_type=MESH,
        )
        for comp in range(3)
    ]
    for comp in range(3):
        loads[comp].wait()
        swap[comp].start()

    def far(p, count):
        at = pl.ds(p, count)
        row = newell_row(other, p)
        return pltpu.make_async_remote_copy(
            src_ref=newell.at[pl.ds(row, 1)] if count == 1 else nwl.at[c, at],
            dst_ref=nwl.at[c, at],
            send_sem=pair_sem.at[1],
            recv_sem=pair_sem.at[2],
            device_id=(g, other),
            device_id_type=MESH,
        )

    for copy in near + late:
        copy.start()
    for p in range(pairs):
        far(p, 1).start()

    for copy in tabs:
        copy.wait()
    def along_z(side, comp):
        return jnp.dot(mag[side, comp], zf[...], preferred_element_type=F32).astype(BF16)

    for comp in range(3):
        zrow[pl.ds(0, rows), pl.ds(2 * comp * half, 2 * half)] = along_z(0, comp)
    own_part = True
    if own_part:
        spec[...] = jnp.dot(yf[:, :rows], zrow[pl.ds(0, rows), :], preferred_element_type=F32)
    for comp in range(3):
        at = pl.ds(2 * comp * half, 2 * half)
        swap[comp].wait_recv()
        far_rows = along_z(1, comp)
        if own_part:
            part = spec[:, at] + jnp.dot(yf[:, rows:], far_rows, preferred_element_type=F32)
        else:
            zrow[pl.ds(rows, rows), at] = far_rows
            part = jnp.dot(yf[...], zrow[:, at], preferred_element_type=F32)
        if whole_tiles:
            for i in range(groups):
                send[i, :, at] = part[i * own : (i + 1) * own].astype(BF16)
        else:
            spec[:, at] = part
    if not whole_tiles:
        for i in range(groups):
            send[i] = spec[pl.ds(i * own, own), :].astype(BF16)

    @pl.when(c == 0)
    def _():
        pl.semaphore_wait(barrier, 2 * (groups - 1))
        pl.semaphore_signal(hand.at[1], inc=1, device_id=(g, 1), device_id_type=MESH)

    @pl.when(c == 1)
    def _():
        pl.semaphore_wait(hand.at[1], 1)

    def forward(to):
        return pltpu.make_async_remote_copy(
            src_ref=send.at[to],
            dst_ref=recv.at[g],
            send_sem=fwd_send.at[0],
            recv_sem=fwd_recv.at[my_layer],
            device_id=(to, c),
            device_id_type=MESH,
        )

    for k in range(1, groups):
        forward(target(k)).start()

    def waiter(ref, send_sem, recv_sem):
        return pltpu.make_async_remote_copy(
            src_ref=ref,
            dst_ref=ref,
            send_sem=send_sem,
            recv_sem=recv_sem,
            device_id=(g, other),
            device_id_type=MESH,
        )

    lane = lax.broadcasted_iota(jnp.int32, (own, half), 1)
    row = lax.broadcasted_iota(jnp.int32, (own, half), 0)
    top = row < pairs

    first_t = (2 * g + c) * pairs + lax.rem(row, pairs)
    al = first_t == 0
    ln = jnp.logical_and(lane == 0, first_t > 0)
    special, ln_low = jnp.logical_or(al, ln), jnp.logical_and(ln, jnp.logical_not(top))

    def flip(v):
        return jnp.concatenate([v[pairs:], v[:pairs]], axis=0)

    def wait_layer(layer):
        sem = fwd_recv.at[layer]

        @pl.when(layer == my_layer)
        def _():
            waiter(recv.at[pl.ds(0, plane - 1)], fwd_send.at[0], sem).wait_recv()

        @pl.when(layer != my_layer)
        def _():
            waiter(recv.at[pl.ds(0, plane)], fwd_send.at[0], sem).wait_recv()

    def unpack(j):
        block = recv[j].astype(F32)
        parts = []
        for comp in range(3):
            re = block[:, 2 * comp * half : (2 * comp + 1) * half]
            im = block[:, (2 * comp + 1) * half : (2 * comp + 2) * half]
            re_f, im_f = flip(re), flip(im)
            new_re = jnp.where(top, re + im_f, re_f - im)
            new_im = jnp.where(top, im - re_f, im_f + re)
            lone_re = jnp.where(ln_low, im_f, re)
            lone_im = jnp.where(al, im, -jnp.where(top, re_f, im))
            parts.append(jnp.where(special, lone_re, new_re))
            parts.append(jnp.where(special, lone_im, new_im))
        return parts

    def k_of(entry, d):
        start = pl.multiple_of((entry * cells + d) * own, own)
        return kern[pl.ds(start, own), :]

    def add_layer(layer, sources, i):
        total = [acc[i, q] for q in range(6)]
        for p in range(plane):
            j = layer * plane + p
            d = jnp.abs(i - j)
            signed = jnp.where(i >= j, 4, 10)
            xx, yy, zz, yz = (k_of(e, d) for e in range(4))
            xy, xz = k_of(signed, d), k_of(signed + 1, d)
            xxi, yyi, zzi, yzi = (k_of(6 + e, d) for e in range(4))
            xr, xi, yr, yim, zr, zim = sources[p]
            total[0] += xx * xr - xy * yim - xz * zim
            total[1] += xxi * xi + xy * yr + xz * zr
            total[2] += yy * yr + yz * zr - xy * xi
            total[3] += yyi * yim + yzi * zim + xy * xr
            total[4] += yz * yr + zz * zr - xz * xi
            total[5] += yzi * yim + zzi * zim + xz * xr
        return total

    def backward(i):
        return pltpu.make_async_remote_copy(
            src_ref=back.at[i],
            dst_ref=fields.at[c, g],
            send_sem=bwd_send.at[0],
            recv_sem=bwd_recv.at[my_layer],
            device_id=(i, c),
            device_id_type=MESH,
        )

    def prepare():
        recv[g] = send[g]
        for copy in near:
            copy.wait()
        far(0, pairs).wait_recv()
        late[0].wait()
        table_rows = 6 * cells
        even_rows = 4 * cells
        lane0 = lax.broadcasted_iota(jnp.int32, (table_rows, half), 1) == 0
        even = lax.broadcasted_iota(jnp.int32, (table_rows, half), 0) < even_rows
        sign = jnp.where(even, 1.0, -1.0).astype(F32)
        row_of = lax.broadcasted_iota(jnp.int32, (table_rows, half), 0)
        diagonal = functools.reduce(jnp.logical_or, [row_of == entry * cells + 1 for entry in range(3)])
        neighbour = jnp.where(diagonal, -2.0 * EXCHANGE, 0.0).astype(F32)
        for p in range(pairs):
            first = nwl[0, p].reshape(table_rows, 2 * half)
            mirror = nwl[1, p].reshape(table_rows, 2 * half)
            rev_first = jnp.dot(first, rv[...], preferred_element_type=F32)
            rev_mirror = jnp.dot(mirror, rv[...], preferred_element_type=F32)
            lo_first, hi_first = first[:, :half].astype(F32), first[:, half:].astype(F32)
            lo_mirror, hi_mirror = mirror[:, :half].astype(F32), mirror[:, half:].astype(F32)
            if p == 0:
                alone = ((2 * g + c) * pairs == 0).astype(F32)
                paired = 1.0 - alone
                of_first = alone * rev_first + paired * rev_mirror
                of_mirror = alone * rev_mirror + paired * rev_first
            else:
                of_first, of_mirror = rev_mirror, rev_first
            k_first = lo_first + sign * of_first
            k_mirror = lo_mirror + sign * of_mirror
            middle = hi_first + sign * hi_mirror
            if p == 0:
                i_first = jnp.where(lane0, alone * (2.0 * hi_first) + paired * k_first, k_first)
                i_mirror = jnp.where(lane0, alone * (2.0 * hi_mirror) + paired * middle, k_mirror)
                k_mirror = jnp.where(lane0, alone * k_mirror + paired * middle, k_mirror)
            else:
                k_mirror = jnp.where(lane0, middle, k_mirror)
                i_first, i_mirror = k_first, k_mirror
            for place, k_all, i_all in ((p, k_first, i_first), (pairs + p, k_mirror, i_mirror)):
                k_all, i_all = k_all + neighbour, i_all + neighbour
                kern[pl.ds(place, table_rows, stride=own), :] = k_all
                kern[pl.ds(table_rows * own + place, even_rows, stride=own), :] = i_all[:even_rows]
                kern[pl.ds((table_rows + even_rows) * own + place, 2 * cells, stride=own), :] = -k_all[even_rows:]
        acc[...] = jnp.zeros(acc.shape, F32)

    def gather(layer):
        wait_layer(layer)
        sources = [unpack(layer * plane + p) for p in range(plane)]

        def over(n, inner):
            for p in range(plane):
                i = n * plane + p
                total = add_layer(layer, sources, i)
                for q in range(6):
                    acc[i, q] = total[q]
            return inner

        lax.fori_loop(0, layers, over, 0)

    def finish(layer):
        wait_layer(layer)
        sources = [unpack(layer * plane + p) for p in range(plane)]

        def dispatch(n):
            for p in range(plane):
                i = target(n * plane + p)

                @pl.when(i != g)
                def _():
                    backward(i).start()

        def over(n, carry):
            for p in range(plane):
                i = target(n * plane + p)
                spread(i, add_layer(layer, sources, i))

            @pl.when(n > 0)
            def _():
                dispatch(jnp.maximum(n - 1, 0))

            return carry

        def spread(i, total):
            for comp in range(3):
                re, im = total[2 * comp], total[2 * comp + 1]
                re_f, im_f = flip(re), flip(im)
                new_re = jnp.where(top, re + re_f, im - im_f)
                new_im = jnp.where(top, im + im_f, re_f - re)
                lone_re = jnp.where(al, re, 2.0 * jnp.where(top, re, -im_f))
                lone_im = jnp.where(al, im, 2.0 * jnp.where(top, re_f, -im))
                new_re = jnp.where(special, lone_re, new_re)
                new_im = jnp.where(special, lone_im, new_im)
                back[i, :, pl.ds(2 * comp * half, half)] = new_re.astype(BF16)
                back[i, :, pl.ds((2 * comp + 1) * half, half)] = new_im.astype(BF16)

        lax.fori_loop(0, layers, over, 0)
        dispatch(layers - 1)
        fields[c, g] = back[g]

    prepare()
    beside = (g > 0).astype(F32) + (g < groups - 1).astype(F32)
    for comp in range(3):
        full = jnp.concatenate([mag[0, comp], mag[1, comp]], axis=0).astype(F32)
        centre = full[:rows]
        total = pltpu.roll(full, 1, 0)[:rows] + pltpu.roll(full, 2 * rows - 1, 0)[:rows]
        total = total + pltpu.roll(centre, 1, 1) + pltpu.roll(centre, 2 * half - 1, 1)
        lap[comp] = EXCHANGE * (total - (4.0 + beside) * centre)

    def step(t, carry):
        gather(group_at(t))
        return carry

    lax.fori_loop(0, layers - 1, step, 0)
    finish(group_at(layers - 1))

    def relay(n):
        return pltpu.make_async_remote_copy(
            src_ref=fields.at[c, pl.ds(n * plane, plane)],
            dst_ref=fields.at[c, pl.ds(n * plane, plane)],
            send_sem=rel_sem.at[0],
            recv_sem=rel_sem.at[1],
            device_id=(g, other),
            device_id_type=MESH,
        )

    for k in range(layers):
        n = relay_at(k)

        @pl.when(n == my_layer)
        def _():
            waiter(fields.at[c, pl.ds(0, plane - 1)], bwd_send.at[0], bwd_recv.at[n]).wait_recv()

        @pl.when(n != my_layer)
        def _():
            waiter(fields.at[c, pl.ds(0, plane)], bwd_send.at[0], bwd_recv.at[n]).wait_recv()

        relay(n).start()

    for copy in late[1:]:
        copy.wait()
    waiter(fields.at[other], rel_sem.at[0], rel_sem.at[1]).wait_recv()

    if whole_tiles:
        modes = fields[...].reshape(2 * groups * own, wide)
    else:
        for part in range(2):
            for i in range(groups):
                stack[pl.ds((part * groups + i) * own, own), :] = fields[part, i].astype(F32)
        modes = stack[...].astype(BF16)
    scale = 1.0 / (2 * rows * 2 * half)
    for comp in range(3):
        at = slice(2 * comp * half, 2 * (comp + 1) * half)
        g_rows = jnp.dot(yi[...], modes[:, at], preferred_element_type=F32).astype(BF16)
        demag = jnp.dot(g_rows, zi[...], preferred_element_type=F32) * scale
        out[comp] = (demag + lap[comp]).astype(BF16)

    waiter(mag.at[0], pair_sem.at[0], swap_recv.at[0]).wait_send()
    waiter(fields.at[c], rel_sem.at[0], rel_sem.at[1]).wait_send()
    far(0, pairs).wait_send()
    waiter(back.at[pl.ds(0, groups - 1)], bwd_send.at[0], bwd_recv.at[0]).wait_send()
    waiter(send.at[pl.ds(0, groups - 1)], fwd_send.at[0], fwd_recv.at[0]).wait_send()


def on_device(magnet, newell, *consts):
    rows, _, x_cells, z_total = magnet.shape
    groups = lax.axis_size("gx")
    parts = lax.axis_size("yz")
    assert x_cells == 1 and parts == 2
    y_total = rows * parts
    pairs = y_total // (groups * parts * 2)
    own = 2 * pairs
    half = z_total // 2
    wide = 3 * z_total
    layers = groups // math.gcd(groups, 4)
    any_ref = pl.BlockSpec(memory_space=pl.ANY)
    dma = pltpu.SemaphoreType.DMA
    planes = jnp.transpose(magnet[:, :, 0, :], (1, 0, 2))
    field = pl.pallas_call(
        functools.partial(kernel, groups, pairs),
        out_shape=pltpu.VMEM(planes.shape, BF16),
        in_specs=[any_ref] * 7,
        out_specs=pl.BlockSpec(memory_space=pltpu.VMEM),
        scratch_shapes=[
            pltpu.VMEM((2, 3, rows, z_total), BF16),
            pltpu.VMEM((2, pairs, 6, groups, z_total), BF16),
            pltpu.VMEM((rows, y_total), BF16),
            pltpu.VMEM((rows, y_total), BF16),
            pltpu.VMEM((z_total, z_total), BF16),
            pltpu.VMEM((z_total, z_total), BF16),
            pltpu.VMEM((z_total, half), BF16),
            pltpu.VMEM((y_total, wide), BF16),
            pltpu.VMEM((rows, wide), F32),
            pltpu.VMEM((groups, own, wide), BF16),
            pltpu.VMEM((groups, own, wide), BF16),
            pltpu.VMEM((12 * groups * own, half), F32),
            pltpu.VMEM((groups, 6, own, half), F32),
            pltpu.VMEM((groups, own, wide), BF16),
            pltpu.VMEM((2, groups, own, wide), BF16),
            pltpu.VMEM((y_total, wide), F32),
            pltpu.VMEM((3, rows, z_total), F32),
            dma((8,)),
            dma((1,)),
            dma((3,)),
            dma((3,)),
            dma((1,)),
            dma((layers,)),
            dma((1,)),
            dma((layers,)),
            dma((2,)),
            pltpu.SemaphoreType.REGULAR((2,)),
        ],
        compiler_params=pltpu.CompilerParams(collective_id=0, has_side_effects=True),
    )(planes, newell, *consts)
    return jnp.transpose(field, (1, 0, 2))[:, :, None, :]


def solution(mesh):
    groups, parts = mesh.shape["gx"], mesh.shape["yz"]

    def run(magnet, newell):
        consts = tables(groups, parts, magnet.shape[0], magnet.shape[3])
        body = lambda m, n: on_device(m, n, *[jnp.asarray(t) for t in consts])
        return jax.shard_map(
            body,
            mesh=mesh,
            in_specs=(P("yz", None, "gx", None), P("yz", None, None, None)),
            out_specs=P("yz", None, "gx", None),
            check_vma=False,
        )(magnet, newell)

    return run
```

```python
import functools
import math

import jax
import jax.numpy as jnp
import ml_dtypes
import numpy as np
from jax import lax
from jax.experimental import pallas as pl
from jax.experimental.pallas import tpu as pltpu
from jax.sharding import PartitionSpec as P

EXCHANGE = 0.2
F32 = jnp.float32
BF16 = jnp.bfloat16
MESH = pl.DeviceIdType.MESH


def tables(groups, parts, y_total, z_total):
    pairs = y_total // (groups * parts * 2)
    rows = y_total // parts
    half_y = y_total // 2

    def trig(k, n, length):
        angle = (k[:, None] * n[None, :] % length) * (2.0 * math.pi / length)
        return np.cos(angle), np.sin(angle)

    def y_rows(part, n):
        blocks = []
        for m in range(groups):
            t = (m * parts + part) * pairs + np.arange(pairs)
            cos, sin = trig(t, n, y_total)
            if t[0] == 0:
                sin[0] = trig(np.array([half_y]), n, y_total)[0][0]
            blocks += [cos, sin]
        return np.concatenate(blocks)

    half = z_total // 2
    cos, sin = trig(np.arange(z_total), np.arange(half), z_total)
    alternate = np.cos(math.pi * np.arange(z_total))
    z_fwd = np.concatenate([cos, -sin], axis=1)
    z_fwd[:, half] = alternate
    z_inv = -np.concatenate([cos, -sin], axis=1).T
    z_inv[0] = -0.5
    z_inv[half] = -0.5 * alternate
    reverse = np.zeros((z_total, half))
    for k in range(half):
        reverse[-k % z_total, k] = 1.0
    forward, inverse = [], []
    for part in range(parts):
        own_first = (np.arange(y_total) + part * rows) % y_total
        forward.append(y_rows(part, own_first))
        inverse.append(np.concatenate([y_rows(other, own_first[:rows]) for other in range(parts)]).T)
    cast = lambda a: np.asarray(a, np.float32).astype(ml_dtypes.bfloat16)
    return cast(np.stack(forward)), cast(np.stack(inverse)), cast(z_fwd), cast(z_inv), cast(reverse)


def kernel(
    groups, pairs, magnet, newell, y_fwd, y_inv, z_fwd, z_inv, rev, out,
    mag, nwl, yf, yi, zf, zi, rv, zrow, spec, send, recv, kern, acc, back, fields, stack,
    lap, load_sem, near_sem, swap_recv, pair_sem, fwd_send, fwd_recv, bwd_send, bwd_recv,
    rel_sem, hand,
):
    g = lax.axis_index("gx")
    c = lax.axis_index("yz")
    other = 1 - c
    own = 2 * pairs
    rows = magnet.shape[1]
    cells = groups
    half = magnet.shape[2] // 2
    wide = 6 * half
    plane = math.gcd(groups, 4)
    layers = groups // plane
    whole_tiles = own % 8 == 0

    my_layer = g // plane

    def is_late(b):
        return b // plane + lax.rem(b, plane) // 2 + lax.rem(b, 2) >= layers + 1

    late_count = sum(int(b // plane + b % plane // 2 + b % 2 >= layers + 1) for b in range(groups))
    lower = g < groups // 2
    low = 2 * my_layer < layers
    from_edge = jnp.where(low, my_layer, layers - 1 - my_layer)

    def layer_at(t):
        v = jnp.where(t <= from_edge, from_edge - t, t)
        return jnp.where(low, v, layers - 1 - v)

    def target(k):
        return lax.rem(g + k, groups)

    def target_back(k):
        zero_at = lax.rem(groups - g, groups)
        return jnp.where(k == 0, 0, jnp.where(k <= zero_at, target(jnp.maximum(k - 1, 0)), target(k)))

    def group_at(t):
        return lax.rem(my_layer + layers - t, layers)

    def relay_at(t):
        return layer_at(t)

    barrier = pltpu.get_barrier_semaphore()
    loads = [
        pltpu.make_async_copy(magnet.at[comp], mag.at[0, comp], load_sem.at[comp]) for comp in range(3)
    ]
    tabs = [
        pltpu.make_async_copy(z_fwd, zf, load_sem.at[3]),
        pltpu.make_async_copy(y_fwd.at[c], yf, load_sem.at[4]),
    ]
    late = [
        pltpu.make_async_copy(rev, rv, load_sem.at[5]),
        pltpu.make_async_copy(y_inv.at[c], yi, load_sem.at[6]),
        pltpu.make_async_copy(z_inv, zi, load_sem.at[7]),
    ]
    for copy in loads:
        copy.start()

    @pl.when(c == 0)
    def _():
        pl.semaphore_signal(barrier, inc=1, device_id=(g, 1), device_id_type=MESH)

    for copy in tabs:
        copy.start()
    for r in range(1, groups):
        to = lax.rem(g + r, groups)

        @pl.when(jnp.logical_or(jnp.logical_not(is_late(g)), to >= groups // 2))
        def _():
            pl.semaphore_signal(barrier, inc=1, device_id=(to, 0), device_id_type=MESH)

    def newell_row(part, p):
        t = (2 * g + part) * pairs + p
        return (1 - c) * t + c * lax.rem(rows - t, rows)

    near = [
        pltpu.make_async_copy(newell.at[newell_row(c, p)], nwl.at[c, p], near_sem.at[0]) for p in range(pairs)
    ]

    @pl.when(c == 1)
    def _():
        pl.semaphore_wait(barrier, 1)
        pl.semaphore_signal(hand.at[0], inc=1, device_id=(g, 0), device_id_type=MESH)

    @pl.when(c == 0)
    def _():
        pl.semaphore_wait(hand.at[0], 1)

    swap = [
        pltpu.make_async_remote_copy(
            src_ref=mag.at[0, comp],
            dst_ref=mag.at[1, comp],
            send_sem=pair_sem.at[0],
            recv_sem=swap_recv.at[comp],
            device_id=(g, other),
            device_id_type=MESH,
        )
        for comp in range(3)
    ]
    for comp in range(3):
        loads[comp].wait()
        swap[comp].start()

    def far(p, count):
        at = pl.ds(p, count)
        row = newell_row(other, p)
        return pltpu.make_async_remote_copy(
            src_ref=newell.at[pl.ds(row, 1)] if count == 1 else nwl.at[c, at],
            dst_ref=nwl.at[c, at],
            send_sem=pair_sem.at[1],
            recv_sem=pair_sem.at[2],
            device_id=(g, other),
            device_id_type=MESH,
        )

    for copy in near + late:
        copy.start()
    for p in range(pairs):
        far(p, 1).start()

    for copy in tabs:
        copy.wait()
    def along_z(side, comp):
        return jnp.dot(mag[side, comp], zf[...], preferred_element_type=F32).astype(BF16)

    for comp in range(3):
        zrow[pl.ds(0, rows), pl.ds(2 * comp * half, 2 * half)] = along_z(0, comp)
    spec[...] = jnp.dot(yf[:, :rows], zrow[pl.ds(0, rows), :], preferred_element_type=F32)
    for copy in swap:
        copy.wait_recv()
    for comp in range(3):
        at = pl.ds(2 * comp * half, 2 * half)
        part = spec[:, at] + jnp.dot(yf[:, rows:], along_z(1, comp), preferred_element_type=F32)
        if whole_tiles:
            for i in range(groups):
                send[i, :, at] = part[i * own : (i + 1) * own].astype(BF16)
        else:
            spec[:, at] = part
    if not whole_tiles:
        for i in range(groups):
            send[i] = spec[pl.ds(i * own, own), :].astype(BF16)

    @pl.when(c == 0)
    def _():
        pl.semaphore_wait(barrier, 2 * (groups - 1 - late_count * lower.astype(jnp.int32)))
        pl.semaphore_signal(hand.at[1], inc=1, device_id=(g, 1), device_id_type=MESH)

        @pl.when(is_late(g))
        def _():
            for to in range(groups // 2):
                for core in range(2):
                    pl.semaphore_signal(hand.at[2], inc=1, device_id=(to, core), device_id_type=MESH)

    @pl.when(c == 1)
    def _():
        pl.semaphore_wait(hand.at[1], 1)

    def forward(to):
        return pltpu.make_async_remote_copy(
            src_ref=send.at[to],
            dst_ref=recv.at[g],
            send_sem=fwd_send.at[0],
            recv_sem=fwd_recv.at[my_layer],
            device_id=(to, c),
            device_id_type=MESH,
        )

    for k in range(1, groups):
        to = target(k)

        @pl.when(jnp.logical_not(jnp.logical_and(lower, is_late(to))))
        def _():
            forward(to).start()

    def waiter(ref, send_sem, recv_sem):
        return pltpu.make_async_remote_copy(
            src_ref=ref,
            dst_ref=ref,
            send_sem=send_sem,
            recv_sem=recv_sem,
            device_id=(g, other),
            device_id_type=MESH,
        )

    lane = lax.broadcasted_iota(jnp.int32, (own, half), 1)
    row = lax.broadcasted_iota(jnp.int32, (own, half), 0)
    top = row < pairs

    first_t = (2 * g + c) * pairs + lax.rem(row, pairs)
    al = first_t == 0
    ln = jnp.logical_and(lane == 0, first_t > 0)
    special, ln_low = jnp.logical_or(al, ln), jnp.logical_and(ln, jnp.logical_not(top))

    def flip(v):
        return jnp.concatenate([v[pairs:], v[:pairs]], axis=0)

    def wait_layer(layer):
        sem = fwd_recv.at[layer]

        @pl.when(layer == my_layer)
        def _():
            waiter(recv.at[pl.ds(0, plane - 1)], fwd_send.at[0], sem).wait_recv()

        @pl.when(layer != my_layer)
        def _():
            waiter(recv.at[pl.ds(0, plane)], fwd_send.at[0], sem).wait_recv()

    def unpack(j):
        block = recv[j].astype(F32)
        parts = []
        for comp in range(3):
            re = block[:, 2 * comp * half : (2 * comp + 1) * half]
            im = block[:, (2 * comp + 1) * half : (2 * comp + 2) * half]
            re_f, im_f = flip(re), flip(im)
            new_re = jnp.where(top, re + im_f, re_f - im)
            new_im = jnp.where(top, im - re_f, im_f + re)
            lone_re = jnp.where(ln_low, im_f, re)
            lone_im = jnp.where(al, im, -jnp.where(top, re_f, im))
            parts.append(jnp.where(special, lone_re, new_re))
            parts.append(jnp.where(special, lone_im, new_im))
        return parts

    def k_of(entry, d):
        start = pl.multiple_of((entry * cells + d) * own, own)
        return kern[pl.ds(start, own), :]

    def add_layer(layer, sources, i):
        total = [acc[i, q] for q in range(6)]
        for p in range(plane):
            j = layer * plane + p
            d = jnp.abs(i - j)
            signed = jnp.where(i >= j, 4, 10)
            xx, yy, zz, yz = (k_of(e, d) for e in range(4))
            xy, xz = k_of(signed, d), k_of(signed + 1, d)
            xxi, yyi, zzi, yzi = (k_of(6 + e, d) for e in range(4))
            xr, xi, yr, yim, zr, zim = sources[p]
            total[0] += xx * xr - xy * yim - xz * zim
            total[1] += xxi * xi + xy * yr + xz * zr
            total[2] += yy * yr + yz * zr - xy * xi
            total[3] += yyi * yim + yzi * zim + xy * xr
            total[4] += yz * yr + zz * zr - xz * xi
            total[5] += yzi * yim + zzi * zim + xz * xr
        return total

    def backward(i):
        return pltpu.make_async_remote_copy(
            src_ref=back.at[i],
            dst_ref=fields.at[c, g],
            send_sem=bwd_send.at[0],
            recv_sem=bwd_recv.at[c * layers + my_layer],
            device_id=(i, 1),
            device_id_type=MESH,
        )

    def prepare():
        recv[g] = send[g]
        for copy in near:
            copy.wait()
        far(0, pairs).wait_recv()
        late[0].wait()
        table_rows = 6 * cells
        even_rows = 4 * cells
        lane0 = lax.broadcasted_iota(jnp.int32, (table_rows, half), 1) == 0
        even = lax.broadcasted_iota(jnp.int32, (table_rows, half), 0) < even_rows
        sign = jnp.where(even, 1.0, -1.0).astype(F32)
        row_of = lax.broadcasted_iota(jnp.int32, (table_rows, half), 0)
        diagonal = functools.reduce(jnp.logical_or, [row_of == entry * cells + 1 for entry in range(3)])
        neighbour = jnp.where(diagonal, -2.0 * EXCHANGE, 0.0).astype(F32)
        for p in range(pairs):
            first = nwl[0, p].reshape(table_rows, 2 * half)
            mirror = nwl[1, p].reshape(table_rows, 2 * half)
            rev_first = jnp.dot(first, rv[...], preferred_element_type=F32)
            rev_mirror = jnp.dot(mirror, rv[...], preferred_element_type=F32)
            lo_first, hi_first = first[:, :half].astype(F32), first[:, half:].astype(F32)
            lo_mirror, hi_mirror = mirror[:, :half].astype(F32), mirror[:, half:].astype(F32)
            if p == 0:
                alone = ((2 * g + c) * pairs == 0).astype(F32)
                paired = 1.0 - alone
                of_first = alone * rev_first + paired * rev_mirror
                of_mirror = alone * rev_mirror + paired * rev_first
            else:
                of_first, of_mirror = rev_mirror, rev_first
            k_first = lo_first + sign * of_first
            k_mirror = lo_mirror + sign * of_mirror
            middle = hi_first + sign * hi_mirror
            if p == 0:
                i_first = jnp.where(lane0, alone * (2.0 * hi_first) + paired * k_first, k_first)
                i_mirror = jnp.where(lane0, alone * (2.0 * hi_mirror) + paired * middle, k_mirror)
                k_mirror = jnp.where(lane0, alone * k_mirror + paired * middle, k_mirror)
            else:
                k_mirror = jnp.where(lane0, middle, k_mirror)
                i_first, i_mirror = k_first, k_mirror
            for place, k_all, i_all in ((p, k_first, i_first), (pairs + p, k_mirror, i_mirror)):
                k_all, i_all = k_all + neighbour, i_all + neighbour
                kern[pl.ds(place, table_rows, stride=own), :] = k_all
                kern[pl.ds(table_rows * own + place, even_rows, stride=own), :] = i_all[:even_rows]
                kern[pl.ds((table_rows + even_rows) * own + place, 2 * cells, stride=own), :] = -k_all[even_rows:]
        acc[...] = jnp.zeros(acc.shape, F32)

    def gather(layer):
        wait_layer(layer)
        sources = [unpack(layer * plane + p) for p in range(plane)]

        def over(n, inner):
            for p in range(plane):
                i = n * plane + p
                total = add_layer(layer, sources, i)
                for q in range(6):
                    acc[i, q] = total[q]
            return inner

        lax.fori_loop(0, layers, over, 0)

    def finish(layer):
        wait_layer(layer)
        sources = [unpack(layer * plane + p) for p in range(plane)]

        chunk = 1

        def dispatch(n):
            for p in range(chunk):
                i = target_back(n * chunk + p)

                @pl.when(i != g)
                def _():
                    backward(i).start()

        def over(n, carry):
            for p in range(chunk):
                i = target_back(n * chunk + p)
                spread(i, add_layer(layer, sources, i))

            @pl.when(n > 0)
            def _():
                dispatch(jnp.maximum(n - 1, 0))

            return carry

        def spread(i, total):
            for comp in range(3):
                re, im = total[2 * comp], total[2 * comp + 1]
                re_f, im_f = flip(re), flip(im)
                new_re = jnp.where(top, re + re_f, im - im_f)
                new_im = jnp.where(top, im + im_f, re_f - re)
                lone_re = jnp.where(al, re, 2.0 * jnp.where(top, re, -im_f))
                lone_im = jnp.where(al, im, 2.0 * jnp.where(top, re_f, -im))
                new_re = jnp.where(special, lone_re, new_re)
                new_im = jnp.where(special, lone_im, new_im)
                back[i, :, pl.ds(2 * comp * half, half)] = new_re.astype(BF16)
                back[i, :, pl.ds((2 * comp + 1) * half, half)] = new_im.astype(BF16)

        lax.fori_loop(0, groups // chunk, over, 0)
        dispatch(groups // chunk - 1)

        @pl.when(c == 1)
        def _():
            fields[1, g] = back[g]

    prepare()
    beside = (g > 0).astype(F32) + (g < groups - 1).astype(F32)
    for comp in range(3):
        full = jnp.concatenate([mag[0, comp], mag[1, comp]], axis=0).astype(F32)
        centre = full[:rows]
        total = pltpu.roll(full, 1, 0)[:rows] + pltpu.roll(full, 2 * rows - 1, 0)[:rows]
        total = total + pltpu.roll(centre, 1, 1) + pltpu.roll(centre, 2 * half - 1, 1)
        lap[comp] = EXCHANGE * (total - (4.0 + beside) * centre)

    if late_count:
        @pl.when(lower)
        def _():
            pl.semaphore_wait(hand.at[2], late_count)
            for k in range(1, groups):
                to = target(k)

                @pl.when(is_late(to))
                def _():
                    forward(to).start()

    def step(t, carry):
        gather(group_at(t))
        return carry

    lax.fori_loop(0, layers - 1, step, 0)
    finish(group_at(layers - 1))

    for copy in late[1:]:
        copy.wait()

    def relay(part, n):
        at = pl.ds(n * plane, plane)
        return pltpu.make_async_remote_copy(
            src_ref=fields.at[part, at],
            dst_ref=fields.at[part, at],
            send_sem=rel_sem.at[0],
            recv_sem=rel_sem.at[1],
            device_id=(g, 0),
            device_id_type=MESH,
        )

    own_block = pltpu.make_async_remote_copy(
        src_ref=back.at[g],
        dst_ref=fields.at[0, g],
        send_sem=bwd_send.at[0],
        recv_sem=bwd_recv.at[my_layer],
        device_id=(g, 1),
        device_id_type=MESH,
    )

    @pl.when(c == 0)
    def _():
        own_block.start()
        waiter(fields, rel_sem.at[0], rel_sem.at[1]).wait_recv()

    @pl.when(c == 1)
    def _():
        for k in range(layers):
            n = relay_at(k)
            for part in (1, 0):
                sem = bwd_recv.at[part * layers + n]
                if part == 1:
                    @pl.when(n == my_layer)
                    def _():
                        waiter(fields.at[1, pl.ds(0, plane - 1)], bwd_send.at[0], sem).wait_recv()

                    @pl.when(n != my_layer)
                    def _():
                        waiter(fields.at[1, pl.ds(0, plane)], bwd_send.at[0], sem).wait_recv()
                else:
                    waiter(fields.at[0, pl.ds(0, plane)], bwd_send.at[0], sem).wait_recv()
                relay(part, n).start()

    if whole_tiles:
        modes = fields[...].reshape(2 * groups * own, wide)
    else:
        for part in range(2):
            for i in range(groups):
                stack[pl.ds((part * groups + i) * own, own), :] = fields[part, i].astype(F32)
        modes = stack[...].astype(BF16)
    scale = 1.0 / (2 * rows * 2 * half)
    for comp in range(3):
        at = slice(2 * comp * half, 2 * (comp + 1) * half)
        g_rows = jnp.dot(yi[...], modes[:, at], preferred_element_type=F32).astype(BF16)
        demag = jnp.dot(g_rows, zi[...], preferred_element_type=F32) * scale
        out[comp] = (demag + lap[comp]).astype(BF16)

    waiter(mag.at[0], pair_sem.at[0], swap_recv.at[0]).wait_send()

    @pl.when(c == 0)
    def _():
        own_block.wait_send()

    @pl.when(c == 1)
    def _():
        waiter(fields, rel_sem.at[0], rel_sem.at[1]).wait_send()

    far(0, pairs).wait_send()
    waiter(back.at[pl.ds(0, groups - 1)], bwd_send.at[0], bwd_recv.at[0]).wait_send()
    waiter(send.at[pl.ds(0, groups - 1)], fwd_send.at[0], fwd_recv.at[0]).wait_send()


def on_device(magnet, newell, *consts):
    rows, _, x_cells, z_total = magnet.shape
    groups = lax.axis_size("gx")
    parts = lax.axis_size("yz")
    assert x_cells == 1 and parts == 2
    y_total = rows * parts
    pairs = y_total // (groups * parts * 2)
    own = 2 * pairs
    half = z_total // 2
    wide = 3 * z_total
    layers = groups // math.gcd(groups, 4)
    any_ref = pl.BlockSpec(memory_space=pl.ANY)
    dma = pltpu.SemaphoreType.DMA
    planes = jnp.transpose(magnet[:, :, 0, :], (1, 0, 2))
    field = pl.pallas_call(
        functools.partial(kernel, groups, pairs),
        out_shape=pltpu.VMEM(planes.shape, BF16),
        in_specs=[any_ref] * 7,
        out_specs=pl.BlockSpec(memory_space=pltpu.VMEM),
        scratch_shapes=[
            pltpu.VMEM((2, 3, rows, z_total), BF16),
            pltpu.VMEM((2, pairs, 6, groups, z_total), BF16),
            pltpu.VMEM((rows, y_total), BF16),
            pltpu.VMEM((rows, y_total), BF16),
            pltpu.VMEM((z_total, z_total), BF16),
            pltpu.VMEM((z_total, z_total), BF16),
            pltpu.VMEM((z_total, half), BF16),
            pltpu.VMEM((y_total, wide), BF16),
            pltpu.VMEM((rows, wide), F32),
            pltpu.VMEM((groups, own, wide), BF16),
            pltpu.VMEM((groups, own, wide), BF16),
            pltpu.VMEM((12 * groups * own, half), F32),
            pltpu.VMEM((groups, 6, own, half), F32),
            pltpu.VMEM((groups, own, wide), BF16),
            pltpu.VMEM((2, groups, own, wide), BF16),
            pltpu.VMEM((y_total, wide), F32),
            pltpu.VMEM((3, rows, z_total), F32),
            dma((8,)),
            dma((1,)),
            dma((3,)),
            dma((3,)),
            dma((1,)),
            dma((layers,)),
            dma((1,)),
            dma((2 * layers,)),
            dma((2,)),
            pltpu.SemaphoreType.REGULAR((3,)),
        ],
        compiler_params=pltpu.CompilerParams(collective_id=0, has_side_effects=True),
    )(planes, newell, *consts)
    return jnp.transpose(field, (1, 0, 2))[:, :, None, :]


def solution(mesh):
    groups, parts = mesh.shape["gx"], mesh.shape["yz"]

    def run(magnet, newell):
        consts = tables(groups, parts, magnet.shape[0], magnet.shape[3])
        body = lambda m, n: on_device(m, n, *[jnp.asarray(t) for t in consts])
        return jax.shard_map(
            body,
            mesh=mesh,
            in_specs=(P("yz", None, "gx", None), P("yz", None, None, None)),
            out_specs=P("yz", None, "gx", None),
            check_vma=False,
        )(magnet, newell)

    return run
```

```python
import functools
import math

import jax
import jax.numpy as jnp
import ml_dtypes
import numpy as np
from jax import lax
from jax.experimental import pallas as pl
from jax.experimental.pallas import tpu as pltpu
from jax.sharding import PartitionSpec as P

EXCHANGE = 0.2
F32 = jnp.float32
BF16 = jnp.bfloat16
MESH = pl.DeviceIdType.MESH


def tables(groups, parts, y_total, z_total):
    pairs = y_total // (groups * parts * 2)
    rows = y_total // parts
    half_y = y_total // 2

    def trig(k, n, length):
        angle = (k[:, None] * n[None, :] % length) * (2.0 * math.pi / length)
        return np.cos(angle), np.sin(angle)

    def y_rows(part, n):
        blocks = []
        for m in range(groups):
            t = (m * parts + part) * pairs + np.arange(pairs)
            cos, sin = trig(t, n, y_total)
            if t[0] == 0:
                sin[0] = trig(np.array([half_y]), n, y_total)[0][0]
            blocks += [cos, sin]
        return np.concatenate(blocks)

    half = z_total // 2
    cos, sin = trig(np.arange(z_total), np.arange(half), z_total)
    alternate = np.cos(math.pi * np.arange(z_total))
    z_fwd = np.concatenate([cos, -sin], axis=1)
    z_fwd[:, half] = alternate
    z_inv = -np.concatenate([cos, -sin], axis=1).T
    z_inv[0] = -0.5
    z_inv[half] = -0.5 * alternate
    reverse = np.zeros((z_total, half))
    for k in range(half):
        reverse[-k % z_total, k] = 1.0
    forward, inverse = [], []
    for part in range(parts):
        own_first = (np.arange(y_total) + part * rows) % y_total
        forward.append(y_rows(part, own_first))
        inverse.append(np.concatenate([y_rows(other, own_first[:rows]) for other in range(parts)]).T)
    cast = lambda a: np.asarray(a, np.float32).astype(ml_dtypes.bfloat16)
    return cast(np.stack(forward)), cast(np.stack(inverse)), cast(z_fwd), cast(z_inv), cast(reverse)


def kernel(
    groups, pairs, magnet, newell, y_fwd, y_inv, z_fwd, z_inv, rev, out,
    mag, nwl, yf, yi, zf, zi, rv, zrow, spec, send, recv, kern, acc, back, fields, stack,
    lap, load_sem, near_sem, swap_recv, pair_sem, fwd_send, fwd_recv, bwd_send, bwd_recv,
    rel_sem, hand,
):
    g = lax.axis_index("gx")
    c = lax.axis_index("yz")
    other = 1 - c
    own = 2 * pairs
    rows = magnet.shape[1]
    cells = groups
    half = magnet.shape[2] // 2
    wide = 6 * half
    plane = math.gcd(groups, 4)
    layers = groups // plane
    whole_tiles = own % 8 == 0

    my_layer = g // plane

    def is_late(b):
        return b // plane + lax.rem(b, plane) // 2 + lax.rem(b, 2) >= layers + 1

    late_count = sum(int(b // plane + b % plane // 2 + b % 2 >= layers + 1) for b in range(groups))
    lower = g < groups // 2
    low = 2 * my_layer < layers
    from_edge = jnp.where(low, my_layer, layers - 1 - my_layer)

    def layer_at(t):
        v = jnp.where(t <= from_edge, from_edge - t, t)
        return jnp.where(low, v, layers - 1 - v)

    def target(k):
        return lax.rem(g + k, groups)

    def target_back(k):
        zero_at = lax.rem(groups - g, groups)
        return jnp.where(k == 0, 0, jnp.where(k <= zero_at, target(jnp.maximum(k - 1, 0)), target(k)))

    def group_at(t):
        return lax.rem(my_layer + layers - t, layers)

    def relay_at(t):
        return layer_at(t)

    barrier = pltpu.get_barrier_semaphore()
    loads = [
        pltpu.make_async_copy(magnet.at[comp], mag.at[0, comp], load_sem.at[comp]) for comp in range(3)
    ]
    tabs = [
        pltpu.make_async_copy(z_fwd, zf, load_sem.at[3]),
        pltpu.make_async_copy(y_fwd.at[c], yf, load_sem.at[4]),
    ]
    late = [
        pltpu.make_async_copy(rev, rv, load_sem.at[5]),
        pltpu.make_async_copy(y_inv.at[c], yi, load_sem.at[6]),
        pltpu.make_async_copy(z_inv, zi, load_sem.at[7]),
    ]
    for copy in loads:
        copy.start()

    @pl.when(c == 0)
    def _():
        pl.semaphore_signal(barrier, inc=1, device_id=(g, 1), device_id_type=MESH)

    for copy in tabs:
        copy.start()
    for r in range(1, groups):
        to = lax.rem(g + r, groups)

        @pl.when(jnp.logical_or(jnp.logical_not(is_late(g)), to >= groups // 2))
        def _():
            pl.semaphore_signal(barrier, inc=1, device_id=(to, 0), device_id_type=MESH)

    def newell_row(part, p):
        t = (2 * g + part) * pairs + p
        return (1 - c) * t + c * lax.rem(rows - t, rows)

    near = [
        pltpu.make_async_copy(newell.at[newell_row(c, p)], nwl.at[c, p], near_sem.at[0]) for p in range(pairs)
    ]

    @pl.when(c == 1)
    def _():
        pl.semaphore_wait(barrier, 1)
        pl.semaphore_signal(hand.at[0], inc=1, device_id=(g, 0), device_id_type=MESH)

    @pl.when(c == 0)
    def _():
        pl.semaphore_wait(hand.at[0], 1)

    swap = [
        pltpu.make_async_remote_copy(
            src_ref=mag.at[0, comp],
            dst_ref=mag.at[1, comp],
            send_sem=pair_sem.at[0],
            recv_sem=swap_recv.at[comp],
            device_id=(g, other),
            device_id_type=MESH,
        )
        for comp in range(3)
    ]
    for comp in range(3):
        loads[comp].wait()
        swap[comp].start()

    def far(p, count):
        at = pl.ds(p, count)
        row = newell_row(other, p)
        return pltpu.make_async_remote_copy(
            src_ref=newell.at[pl.ds(row, 1)] if count == 1 else nwl.at[c, at],
            dst_ref=nwl.at[c, at],
            send_sem=pair_sem.at[1],
            recv_sem=pair_sem.at[2],
            device_id=(g, other),
            device_id_type=MESH,
        )

    for copy in near + late:
        copy.start()
    for p in range(pairs):
        far(p, 1).start()

    def meet():
        @pl.when(c == 0)
        def _():
            pl.semaphore_wait(barrier, 2 * (groups - 1 - late_count * lower.astype(jnp.int32)))

            @pl.when(is_late(g))
            def _():
                for to in range(groups // 2):
                    for core in range(2):
                        pl.semaphore_signal(hand.at[2], inc=1, device_id=(to, core), device_id_type=MESH)

            pl.semaphore_signal(hand.at[1], inc=1, device_id=(g, 1), device_id_type=MESH)

        @pl.when(c == 1)
        def _():
            pl.semaphore_wait(hand.at[1], 1)

    for copy in tabs:
        copy.wait()
    def along_z(side, comp):
        return jnp.dot(mag[side, comp], zf[...], preferred_element_type=F32).astype(BF16)

    for comp in range(3):
        zrow[pl.ds(0, rows), pl.ds(2 * comp * half, 2 * half)] = along_z(0, comp)
    spec[...] = jnp.dot(yf[:, :rows], zrow[pl.ds(0, rows), :], preferred_element_type=F32)
    @pl.when(is_late(g))
    def _():
        meet()

    for copy in swap:
        copy.wait_recv()
    for comp in range(3):
        at = pl.ds(2 * comp * half, 2 * half)
        part = spec[:, at] + jnp.dot(yf[:, rows:], along_z(1, comp), preferred_element_type=F32)
        if whole_tiles:
            for i in range(groups):
                send[i, :, at] = part[i * own : (i + 1) * own].astype(BF16)
        else:
            spec[:, at] = part
    if not whole_tiles:
        for i in range(groups):
            send[i] = spec[pl.ds(i * own, own), :].astype(BF16)

    @pl.when(jnp.logical_not(is_late(g)))
    def _():
        meet()

    def forward(to):
        return pltpu.make_async_remote_copy(
            src_ref=send.at[to],
            dst_ref=recv.at[g],
            send_sem=fwd_send.at[0],
            recv_sem=fwd_recv.at[my_layer],
            device_id=(to, c),
            device_id_type=MESH,
        )

    for k in range(1, groups):
        to = target(k)

        @pl.when(jnp.logical_not(jnp.logical_and(lower, is_late(to))))
        def _():
            forward(to).start()

    def waiter(ref, send_sem, recv_sem):
        return pltpu.make_async_remote_copy(
            src_ref=ref,
            dst_ref=ref,
            send_sem=send_sem,
            recv_sem=recv_sem,
            device_id=(g, other),
            device_id_type=MESH,
        )

    lane = lax.broadcasted_iota(jnp.int32, (own, half), 1)
    row = lax.broadcasted_iota(jnp.int32, (own, half), 0)
    top = row < pairs

    first_t = (2 * g + c) * pairs + lax.rem(row, pairs)
    al = first_t == 0
    ln = jnp.logical_and(lane == 0, first_t > 0)
    special, ln_low = jnp.logical_or(al, ln), jnp.logical_and(ln, jnp.logical_not(top))

    def flip(v):
        return jnp.concatenate([v[pairs:], v[:pairs]], axis=0)

    def wait_layer(layer):
        sem = fwd_recv.at[layer]

        @pl.when(layer == my_layer)
        def _():
            waiter(recv.at[pl.ds(0, plane - 1)], fwd_send.at[0], sem).wait_recv()

        @pl.when(layer != my_layer)
        def _():
            waiter(recv.at[pl.ds(0, plane)], fwd_send.at[0], sem).wait_recv()

    def unpack(j):
        block = recv[j].astype(F32)
        parts = []
        for comp in range(3):
            re = block[:, 2 * comp * half : (2 * comp + 1) * half]
            im = block[:, (2 * comp + 1) * half : (2 * comp + 2) * half]
            re_f, im_f = flip(re), flip(im)
            new_re = jnp.where(top, re + im_f, re_f - im)
            new_im = jnp.where(top, im - re_f, im_f + re)
            lone_re = jnp.where(ln_low, im_f, re)
            lone_im = jnp.where(al, im, -jnp.where(top, re_f, im))
            parts.append(jnp.where(special, lone_re, new_re))
            parts.append(jnp.where(special, lone_im, new_im))
        return parts

    def k_of(entry, d):
        start = pl.multiple_of((entry * cells + d) * own, own)
        return kern[pl.ds(start, own), :]

    def add_layer(layer, sources, i):
        total = [acc[i, q] for q in range(6)]
        for p in range(plane):
            j = layer * plane + p
            d = jnp.abs(i - j)
            signed = jnp.where(i >= j, 4, 10)
            xx, yy, zz, yz = (k_of(e, d) for e in range(4))
            xy, xz = k_of(signed, d), k_of(signed + 1, d)
            xxi, yyi, zzi, yzi = (k_of(6 + e, d) for e in range(4))
            xr, xi, yr, yim, zr, zim = sources[p]
            total[0] += xx * xr - xy * yim - xz * zim
            total[1] += xxi * xi + xy * yr + xz * zr
            total[2] += yy * yr + yz * zr - xy * xi
            total[3] += yyi * yim + yzi * zim + xy * xr
            total[4] += yz * yr + zz * zr - xz * xi
            total[5] += yzi * yim + zzi * zim + xz * xr
        return total

    def backward(i, core=1):
        return pltpu.make_async_remote_copy(
            src_ref=back.at[i],
            dst_ref=fields.at[c, g],
            send_sem=bwd_send.at[0],
            recv_sem=bwd_recv.at[c * layers + my_layer],
            device_id=(i, core),
            device_id_type=MESH,
        )

    direct = layers - 1
    twice = jnp.logical_and(c == 0, my_layer == direct)

    def prepare():
        recv[g] = send[g]
        for copy in near:
            copy.wait()
        far(0, pairs).wait_recv()
        late[0].wait()
        table_rows = 6 * cells
        even_rows = 4 * cells
        lane0 = lax.broadcasted_iota(jnp.int32, (table_rows, half), 1) == 0
        even = lax.broadcasted_iota(jnp.int32, (table_rows, half), 0) < even_rows
        sign = jnp.where(even, 1.0, -1.0).astype(F32)
        row_of = lax.broadcasted_iota(jnp.int32, (table_rows, half), 0)
        diagonal = functools.reduce(jnp.logical_or, [row_of == entry * cells + 1 for entry in range(3)])
        neighbour = jnp.where(diagonal, -2.0 * EXCHANGE, 0.0).astype(F32)
        for p in range(pairs):
            first = nwl[0, p].reshape(table_rows, 2 * half)
            mirror = nwl[1, p].reshape(table_rows, 2 * half)
            rev_first = jnp.dot(first, rv[...], preferred_element_type=F32)
            rev_mirror = jnp.dot(mirror, rv[...], preferred_element_type=F32)
            lo_first, hi_first = first[:, :half].astype(F32), first[:, half:].astype(F32)
            lo_mirror, hi_mirror = mirror[:, :half].astype(F32), mirror[:, half:].astype(F32)
            if p == 0:
                alone = ((2 * g + c) * pairs == 0).astype(F32)
                paired = 1.0 - alone
                of_first = alone * rev_first + paired * rev_mirror
                of_mirror = alone * rev_mirror + paired * rev_first
            else:
                of_first, of_mirror = rev_mirror, rev_first
            k_first = lo_first + sign * of_first
            k_mirror = lo_mirror + sign * of_mirror
            middle = hi_first + sign * hi_mirror
            if p == 0:
                i_first = jnp.where(lane0, alone * (2.0 * hi_first) + paired * k_first, k_first)
                i_mirror = jnp.where(lane0, alone * (2.0 * hi_mirror) + paired * middle, k_mirror)
                k_mirror = jnp.where(lane0, alone * k_mirror + paired * middle, k_mirror)
            else:
                k_mirror = jnp.where(lane0, middle, k_mirror)
                i_first, i_mirror = k_first, k_mirror
            for place, k_all, i_all in ((p, k_first, i_first), (pairs + p, k_mirror, i_mirror)):
                k_all, i_all = k_all + neighbour, i_all + neighbour
                kern[pl.ds(place, table_rows, stride=own), :] = k_all
                kern[pl.ds(table_rows * own + place, even_rows, stride=own), :] = i_all[:even_rows]
                kern[pl.ds((table_rows + even_rows) * own + place, 2 * cells, stride=own), :] = -k_all[even_rows:]
        acc[...] = jnp.zeros(acc.shape, F32)

    def gather(layer):
        wait_layer(layer)
        sources = [unpack(layer * plane + p) for p in range(plane)]

        def over(n, inner):
            for p in range(plane):
                i = n * plane + p
                total = add_layer(layer, sources, i)
                for q in range(6):
                    acc[i, q] = total[q]
            return inner

        lax.fori_loop(0, layers, over, 0)

    def finish(layer):
        wait_layer(layer)
        sources = [unpack(layer * plane + p) for p in range(plane)]


        def dispatch(n):
            i = target_back(n)

            @pl.when(i != g)
            def _():
                backward(i).start()

            @pl.when(jnp.logical_and(i == 0, twice))
            def _():
                backward(i, 0).start()

        def over(n, carry):
            i = target_back(n)
            spread(i, add_layer(layer, sources, i))

            @pl.when(n > 0)
            def _():
                dispatch(jnp.maximum(n - 1, 0))

            return carry

        def spread(i, total):
            for comp in range(3):
                re, im = total[2 * comp], total[2 * comp + 1]
                re_f, im_f = flip(re), flip(im)
                new_re = jnp.where(top, re + re_f, im - im_f)
                new_im = jnp.where(top, im + im_f, re_f - re)
                lone_re = jnp.where(al, re, 2.0 * jnp.where(top, re, -im_f))
                lone_im = jnp.where(al, im, 2.0 * jnp.where(top, re_f, -im))
                new_re = jnp.where(special, lone_re, new_re)
                new_im = jnp.where(special, lone_im, new_im)
                back[i, :, pl.ds(2 * comp * half, half)] = new_re.astype(BF16)
                back[i, :, pl.ds((2 * comp + 1) * half, half)] = new_im.astype(BF16)

        lax.fori_loop(0, groups, over, 0)
        dispatch(groups - 1)

        @pl.when(c == 1)
        def _():
            fields[1, g] = back[g]

    prepare()
    beside = (g > 0).astype(F32) + (g < groups - 1).astype(F32)
    for comp in range(3):
        full = jnp.concatenate([mag[0, comp], mag[1, comp]], axis=0).astype(F32)
        centre = full[:rows]
        total = pltpu.roll(full, 1, 0)[:rows] + pltpu.roll(full, 2 * rows - 1, 0)[:rows]
        total = total + pltpu.roll(centre, 1, 1) + pltpu.roll(centre, 2 * half - 1, 1)
        lap[comp] = EXCHANGE * (total - (4.0 + beside) * centre)

    if late_count:
        @pl.when(lower)
        def _():
            pl.semaphore_wait(hand.at[2], late_count)
            for k in range(1, groups):
                to = target(k)

                @pl.when(is_late(to))
                def _():
                    forward(to).start()

    def step(t, carry):
        gather(group_at(t))
        return carry

    lax.fori_loop(0, layers - 1, step, 0)
    finish(group_at(layers - 1))

    for copy in late[1:]:
        copy.wait()

    def relay(part, n):
        at = pl.ds(n * plane, plane)
        return pltpu.make_async_remote_copy(
            src_ref=fields.at[part, at],
            dst_ref=fields.at[part, at],
            send_sem=rel_sem.at[0],
            recv_sem=rel_sem.at[1],
            device_id=(g, 0),
            device_id_type=MESH,
        )

    own_block = pltpu.make_async_remote_copy(
        src_ref=back.at[g],
        dst_ref=fields.at[0, g],
        send_sem=bwd_send.at[0],
        recv_sem=bwd_recv.at[my_layer],
        device_id=(g, 1),
        device_id_type=MESH,
    )

    @pl.when(c == 0)
    def _():
        own_block.start()

        @pl.when(g == 0)
        def _():
            waiter(fields.at[:, pl.ds(0, groups - plane // 2)], rel_sem.at[0], rel_sem.at[1]).wait_recv()
            at = pl.ds(direct * plane, plane)
            waiter(fields.at[0, at], bwd_send.at[0], bwd_recv.at[direct]).wait_recv()

        @pl.when(g != 0)
        def _():
            waiter(fields, rel_sem.at[0], rel_sem.at[1]).wait_recv()

    @pl.when(c == 1)
    def _():
        for k in range(layers):
            n = relay_at(k)
            for part in (1, 0):
                sem = bwd_recv.at[part * layers + n]
                if part == 1:
                    @pl.when(n == my_layer)
                    def _():
                        waiter(fields.at[1, pl.ds(0, plane - 1)], bwd_send.at[0], sem).wait_recv()

                    @pl.when(n != my_layer)
                    def _():
                        waiter(fields.at[1, pl.ds(0, plane)], bwd_send.at[0], sem).wait_recv()
                else:
                    waiter(fields.at[0, pl.ds(0, plane)], bwd_send.at[0], sem).wait_recv()
                if part == 1:
                    relay(part, n).start()
                else:
                    @pl.when(jnp.logical_or(g != 0, n != direct))
                    def _():
                        relay(part, n).start()

    if whole_tiles:
        modes = fields[...].reshape(2 * groups * own, wide)
    else:
        for part in range(2):
            for i in range(groups):
                stack[pl.ds((part * groups + i) * own, own), :] = fields[part, i].astype(F32)
        modes = stack[...].astype(BF16)
    scale = 1.0 / (2 * rows * 2 * half)
    for comp in range(3):
        at = slice(2 * comp * half, 2 * (comp + 1) * half)
        g_rows = jnp.dot(yi[...], modes[:, at], preferred_element_type=F32).astype(BF16)
        demag = jnp.dot(g_rows, zi[...], preferred_element_type=F32) * scale
        out[comp] = (demag + lap[comp]).astype(BF16)

    waiter(mag.at[0], pair_sem.at[0], swap_recv.at[0]).wait_send()

    @pl.when(c == 0)
    def _():
        own_block.wait_send()

    @pl.when(twice)
    def _():
        backward(0, 0).wait_send()

    @pl.when(c == 1)
    def _():
        @pl.when(g == 0)
        def _():
            waiter(fields.at[:, pl.ds(0, groups - plane // 2)], rel_sem.at[0], rel_sem.at[1]).wait_send()

        @pl.when(g != 0)
        def _():
            waiter(fields, rel_sem.at[0], rel_sem.at[1]).wait_send()

    far(0, pairs).wait_send()
    waiter(back.at[pl.ds(0, groups - 1)], bwd_send.at[0], bwd_recv.at[0]).wait_send()
    waiter(send.at[pl.ds(0, groups - 1)], fwd_send.at[0], fwd_recv.at[0]).wait_send()


def on_device(magnet, newell, *consts):
    rows, _, x_cells, z_total = magnet.shape
    groups = lax.axis_size("gx")
    parts = lax.axis_size("yz")
    assert x_cells == 1 and parts == 2
    y_total = rows * parts
    pairs = y_total // (groups * parts * 2)
    own = 2 * pairs
    half = z_total // 2
    wide = 3 * z_total
    layers = groups // math.gcd(groups, 4)
    any_ref = pl.BlockSpec(memory_space=pl.ANY)
    dma = pltpu.SemaphoreType.DMA
    planes = jnp.transpose(magnet[:, :, 0, :], (1, 0, 2))
    field = pl.pallas_call(
        functools.partial(kernel, groups, pairs),
        out_shape=pltpu.VMEM(planes.shape, BF16),
        in_specs=[any_ref] * 7,
        out_specs=pl.BlockSpec(memory_space=pltpu.VMEM),
        scratch_shapes=[
            pltpu.VMEM((2, 3, rows, z_total), BF16),
            pltpu.VMEM((2, pairs, 6, groups, z_total), BF16),
            pltpu.VMEM((rows, y_total), BF16),
            pltpu.VMEM((rows, y_total), BF16),
            pltpu.VMEM((z_total, z_total), BF16),
            pltpu.VMEM((z_total, z_total), BF16),
            pltpu.VMEM((z_total, half), BF16),
            pltpu.VMEM((y_total, wide), BF16),
            pltpu.VMEM((rows, wide), F32),
            pltpu.VMEM((groups, own, wide), BF16),
            pltpu.VMEM((groups, own, wide), BF16),
            pltpu.VMEM((12 * groups * own, half), F32),
            pltpu.VMEM((groups, 6, own, half), F32),
            pltpu.VMEM((groups, own, wide), BF16),
            pltpu.VMEM((2, groups, own, wide), BF16),
            pltpu.VMEM((y_total, wide), F32),
            pltpu.VMEM((3, rows, z_total), F32),
            dma((8,)),
            dma((1,)),
            dma((3,)),
            dma((3,)),
            dma((1,)),
            dma((layers,)),
            dma((1,)),
            dma((2 * layers,)),
            dma((2,)),
            pltpu.SemaphoreType.REGULAR((3,)),
        ],
        compiler_params=pltpu.CompilerParams(collective_id=0, has_side_effects=True),
    )(planes, newell, *consts)
    return jnp.transpose(field, (1, 0, 2))[:, :, None, :]


def solution(mesh):
    groups, parts = mesh.shape["gx"], mesh.shape["yz"]

    def run(magnet, newell):
        consts = tables(groups, parts, magnet.shape[0], magnet.shape[3])
        body = lambda m, n: on_device(m, n, *[jnp.asarray(t) for t in consts])
        return jax.shard_map(
            body,
            mesh=mesh,
            in_specs=(P("yz", None, "gx", None), P("yz", None, None, None)),
            out_specs=P("yz", None, "gx", None),
            check_vma=False,
        )(magnet, newell)

    return run
```

```python
import functools
import math

import jax
import jax.numpy as jnp
import ml_dtypes
import numpy as np
from jax import lax
from jax.experimental import pallas as pl
from jax.experimental.pallas import tpu as pltpu
from jax.sharding import PartitionSpec as P

EXCHANGE = 0.2
F32 = jnp.float32
BF16 = jnp.bfloat16
MESH = pl.DeviceIdType.MESH


def tables(groups, parts, y_total, z_total):
    pairs = y_total // (groups * parts * 2)
    rows = y_total // parts
    half_y = y_total // 2

    def trig(k, n, length):
        angle = (k[:, None] * n[None, :] % length) * (2.0 * math.pi / length)
        return np.cos(angle), np.sin(angle)

    def y_rows(part, n):
        blocks = []
        for m in range(groups):
            t = (m * parts + part) * pairs + np.arange(pairs)
            cos, sin = trig(t, n, y_total)
            if t[0] == 0:
                sin[0] = trig(np.array([half_y]), n, y_total)[0][0]
            blocks += [cos, sin]
        return np.concatenate(blocks)

    half = z_total // 2
    cos, sin = trig(np.arange(z_total), np.arange(half), z_total)
    alternate = np.cos(math.pi * np.arange(z_total))
    z_fwd = np.concatenate([cos, -sin], axis=1)
    z_fwd[:, half] = alternate
    z_inv = -np.concatenate([cos, -sin], axis=1).T
    z_inv[0] = -0.5
    z_inv[half] = -0.5 * alternate
    reverse = np.zeros((z_total, half))
    for k in range(half):
        reverse[-k % z_total, k] = 1.0
    forward, inverse = [], []
    for part in range(parts):
        own_first = (np.arange(y_total) + part * rows) % y_total
        forward.append(y_rows(part, own_first))
        inverse.append(np.concatenate([y_rows(other, own_first[:rows]) for other in range(parts)]).T)
    cast = lambda a: np.asarray(a, np.float32).astype(ml_dtypes.bfloat16)
    return cast(np.stack(forward)), cast(np.stack(inverse)), cast(z_fwd), cast(z_inv), cast(reverse)


def kernel(
    groups, pairs, magnet, newell, y_fwd, y_inv, z_fwd, z_inv, rev, out,
    mag, nwl, yf, yi, zf, zi, rv, zrow, spec, send, recv, kern, acc, back, fields, stack,
    lap, load_sem, near_sem, swap_recv, pair_sem, fwd_send, fwd_recv, bwd_send, bwd_recv,
    rel_sem, hand,
):
    g = lax.axis_index("gx")
    c = lax.axis_index("yz")
    other = 1 - c
    own = 2 * pairs
    rows = magnet.shape[1]
    cells = groups
    half = magnet.shape[2] // 2
    wide = 6 * half
    plane = math.gcd(groups, 4)
    layers = groups // plane
    whole_tiles = own % 8 == 0

    my_layer = g // plane

    def is_late(b):
        return b // plane + lax.rem(b, plane) // 2 + lax.rem(b, 2) >= layers + 1

    late_count = sum(int(b // plane + b % plane // 2 + b % 2 >= layers + 1) for b in range(groups))
    lower = g < groups // 2
    low = 2 * my_layer < layers
    from_edge = jnp.where(low, my_layer, layers - 1 - my_layer)

    def layer_at(t):
        v = jnp.where(t <= from_edge, from_edge - t, t)
        return jnp.where(low, v, layers - 1 - v)

    def target(k):
        return lax.rem(g + k, groups)

    def target_back(k):
        zero_at = lax.rem(groups - g, groups)
        return jnp.where(k == 0, 0, jnp.where(k <= zero_at, target(jnp.maximum(k - 1, 0)), target(k)))

    def group_at(t):
        return lax.rem(my_layer + layers - t, layers)

    def relay_at(t):
        return jnp.where(jnp.logical_and(my_layer == layers - 1, t >= 2), t - 2, jnp.where(t <= my_layer, my_layer - t, t))

    barrier = pltpu.get_barrier_semaphore()
    loads = [
        pltpu.make_async_copy(magnet.at[comp], mag.at[0, comp], load_sem.at[0]) for comp in range(3)
    ]
    tabs = [
        pltpu.make_async_copy(z_fwd, zf, load_sem.at[1]),
        pltpu.make_async_copy(y_fwd.at[c], yf, load_sem.at[2]),
    ]
    late = [
        pltpu.make_async_copy(rev, rv, load_sem.at[3]),
        pltpu.make_async_copy(y_inv.at[c], yi, load_sem.at[4]),
        pltpu.make_async_copy(z_inv, zi, load_sem.at[5]),
    ]
    for copy in loads:
        copy.start()

    @pl.when(c == 0)
    def _():
        pl.semaphore_signal(barrier, inc=1, device_id=(g, 1), device_id_type=MESH)

    for copy in tabs:
        copy.start()
    for r in range(1, groups):
        to = lax.rem(g + r, groups)

        @pl.when(jnp.logical_or(jnp.logical_not(is_late(g)), to >= groups // 2))
        def _():
            pl.semaphore_signal(barrier, inc=1, device_id=(to, 0), device_id_type=MESH)

    def newell_row(part, p):
        t = (2 * g + part) * pairs + p
        return (1 - c) * t + c * lax.rem(rows - t, rows)

    near = [
        pltpu.make_async_copy(newell.at[newell_row(c, p)], nwl.at[c, p], near_sem.at[0]) for p in range(pairs)
    ]

    def waiter(ref, send_sem, recv_sem):
        return pltpu.make_async_remote_copy(
            src_ref=ref,
            dst_ref=ref,
            send_sem=send_sem,
            recv_sem=recv_sem,
            device_id=(g, other),
            device_id_type=MESH,
        )

    @pl.when(c == 1)
    def _():
        pl.semaphore_wait(barrier, 1)
        pl.semaphore_signal(hand.at[0], inc=1, device_id=(g, 0), device_id_type=MESH)

    @pl.when(c == 0)
    def _():
        pl.semaphore_wait(hand.at[0], 1)

    def meet():
        @pl.when(c == 0)
        def _():
            pl.semaphore_wait(barrier, 2 * (groups - 1 - late_count * lower.astype(jnp.int32)))

            @pl.when(is_late(g))
            def _():
                for to in range(groups // 2):
                    for core in range(2):
                        pl.semaphore_signal(hand.at[2], inc=1, device_id=(to, core), device_id_type=MESH)

            pl.semaphore_signal(hand.at[1], inc=1, device_id=(g, 1), device_id_type=MESH)

        @pl.when(c == 1)
        def _():
            pl.semaphore_wait(hand.at[1], 1)

    @pl.when(is_late(g))
    def _():
        meet()

    swap = [
        pltpu.make_async_remote_copy(
            src_ref=mag.at[0, comp],
            dst_ref=mag.at[1, comp],
            send_sem=pair_sem.at[0],
            recv_sem=swap_recv.at[0],
            device_id=(g, other),
            device_id_type=MESH,
        )
        for comp in range(3)
    ]
    pltpu.make_async_copy(mag.at[0], mag.at[0], load_sem.at[0]).wait()
    for copy in swap:
        copy.start()

    def far(p, count):
        at = pl.ds(p, count)
        row = newell_row(other, p)
        return pltpu.make_async_remote_copy(
            src_ref=newell.at[pl.ds(row, 1)] if count == 1 else nwl.at[c, at],
            dst_ref=nwl.at[c, at],
            send_sem=pair_sem.at[1],
            recv_sem=pair_sem.at[2],
            device_id=(g, other),
            device_id_type=MESH,
        )

    for copy in near + late:
        copy.start()
    for p in range(pairs):
        far(p, 1).start()

    for copy in tabs:
        copy.wait()
    def along_z(side, comp):
        return jnp.dot(mag[side, comp], zf[...], preferred_element_type=F32).astype(BF16)

    for comp in range(3):
        zrow[pl.ds(0, rows), pl.ds(2 * comp * half, 2 * half)] = along_z(0, comp)
    spec[...] = jnp.dot(yf[:, :rows], zrow[pl.ds(0, rows), :], preferred_element_type=F32)
    waiter(mag.at[1], pair_sem.at[0], swap_recv.at[0]).wait_recv()
    for comp in range(3):
        at = pl.ds(2 * comp * half, 2 * half)
        part = spec[:, at] + jnp.dot(yf[:, rows:], along_z(1, comp), preferred_element_type=F32)
        if whole_tiles:
            for i in range(groups):
                send[i, :, at] = part[i * own : (i + 1) * own].astype(BF16)
        else:
            spec[:, at] = part
    if not whole_tiles:
        for i in range(groups):
            send[i] = spec[pl.ds(i * own, own), :].astype(BF16)

    @pl.when(jnp.logical_not(is_late(g)))
    def _():
        meet()

    def forward(to):
        return pltpu.make_async_remote_copy(
            src_ref=send.at[to],
            dst_ref=recv.at[g],
            send_sem=fwd_send.at[0],
            recv_sem=fwd_recv.at[my_layer],
            device_id=(to, c),
            device_id_type=MESH,
        )

    for k in range(1, groups):
        to = target(k)

        @pl.when(jnp.logical_not(jnp.logical_and(lower, is_late(to))))
        def _():
            forward(to).start()

    lane = lax.broadcasted_iota(jnp.int32, (own, half), 1)
    row = lax.broadcasted_iota(jnp.int32, (own, half), 0)
    top = row < pairs

    first_t = (2 * g + c) * pairs + lax.rem(row, pairs)
    al = first_t == 0
    ln = jnp.logical_and(lane == 0, first_t > 0)
    special, ln_low = jnp.logical_or(al, ln), jnp.logical_and(ln, jnp.logical_not(top))

    def flip(v):
        return jnp.concatenate([v[pairs:], v[:pairs]], axis=0)

    def wait_layer(layer):
        sem = fwd_recv.at[layer]

        @pl.when(layer == my_layer)
        def _():
            waiter(recv.at[pl.ds(0, plane - 1)], fwd_send.at[0], sem).wait_recv()

        @pl.when(layer != my_layer)
        def _():
            waiter(recv.at[pl.ds(0, plane)], fwd_send.at[0], sem).wait_recv()

    def unpack(j):
        block = recv[j].astype(F32)
        parts = []
        for comp in range(3):
            re = block[:, 2 * comp * half : (2 * comp + 1) * half]
            im = block[:, (2 * comp + 1) * half : (2 * comp + 2) * half]
            re_f, im_f = flip(re), flip(im)
            new_re = jnp.where(top, re + im_f, re_f - im)
            new_im = jnp.where(top, im - re_f, im_f + re)
            lone_re = jnp.where(ln_low, im_f, re)
            lone_im = jnp.where(al, im, -jnp.where(top, re_f, im))
            parts.append(jnp.where(special, lone_re, new_re))
            parts.append(jnp.where(special, lone_im, new_im))
        return parts

    def k_of(entry, d):
        start = pl.multiple_of((entry * cells + d) * own, own)
        return kern[pl.ds(start, own), :]

    def add_layer(layer, sources, i):
        total = [acc[i, q] for q in range(6)]
        for p in range(plane):
            j = layer * plane + p
            d = jnp.abs(i - j)
            signed = jnp.where(i >= j, 4, 10)
            xx, yy, zz, yz = (k_of(e, d) for e in range(4))
            xy, xz = k_of(signed, d), k_of(signed + 1, d)
            xxi, yyi, zzi, yzi = (k_of(6 + e, d) for e in range(4))
            xr, xi, yr, yim, zr, zim = sources[p]
            total[0] += xx * xr - xy * yim - xz * zim
            total[1] += xxi * xi + xy * yr + xz * zr
            total[2] += yy * yr + yz * zr - xy * xi
            total[3] += yyi * yim + yzi * zim + xy * xr
            total[4] += yz * yr + zz * zr - xz * xi
            total[5] += yzi * yim + zzi * zim + xz * xr
        return total

    def backward(i, core=1):
        return pltpu.make_async_remote_copy(
            src_ref=back.at[i],
            dst_ref=fields.at[c, g],
            send_sem=bwd_send.at[0],
            recv_sem=bwd_recv.at[c * layers + my_layer],
            device_id=(i, core),
            device_id_type=MESH,
        )

    direct = layers - 1
    twice = jnp.logical_and(c == 0, my_layer == direct)

    def prepare():
        recv[g] = send[g]
        for copy in near:
            copy.wait()
        far(0, pairs).wait_recv()
        late[0].wait()
        table_rows = 6 * cells
        even_rows = 4 * cells
        lane0 = lax.broadcasted_iota(jnp.int32, (table_rows, half), 1) == 0
        even = lax.broadcasted_iota(jnp.int32, (table_rows, half), 0) < even_rows
        sign = jnp.where(even, 1.0, -1.0).astype(F32)
        row_of = lax.broadcasted_iota(jnp.int32, (table_rows, half), 0)
        diagonal = functools.reduce(jnp.logical_or, [row_of == entry * cells + 1 for entry in range(3)])
        neighbour = jnp.where(diagonal, -2.0 * EXCHANGE, 0.0).astype(F32)
        for p in range(pairs):
            first = nwl[0, p].reshape(table_rows, 2 * half)
            mirror = nwl[1, p].reshape(table_rows, 2 * half)
            rev_first = jnp.dot(first, rv[...], preferred_element_type=F32)
            rev_mirror = jnp.dot(mirror, rv[...], preferred_element_type=F32)
            lo_first, hi_first = first[:, :half].astype(F32), first[:, half:].astype(F32)
            lo_mirror, hi_mirror = mirror[:, :half].astype(F32), mirror[:, half:].astype(F32)
            if p == 0:
                alone = ((2 * g + c) * pairs == 0).astype(F32)
                paired = 1.0 - alone
                of_first = alone * rev_first + paired * rev_mirror
                of_mirror = alone * rev_mirror + paired * rev_first
            else:
                of_first, of_mirror = rev_mirror, rev_first
            k_first = lo_first + sign * of_first
            k_mirror = lo_mirror + sign * of_mirror
            middle = hi_first + sign * hi_mirror
            if p == 0:
                i_first = jnp.where(lane0, alone * (2.0 * hi_first) + paired * k_first, k_first)
                i_mirror = jnp.where(lane0, alone * (2.0 * hi_mirror) + paired * middle, k_mirror)
                k_mirror = jnp.where(lane0, alone * k_mirror + paired * middle, k_mirror)
            else:
                k_mirror = jnp.where(lane0, middle, k_mirror)
                i_first, i_mirror = k_first, k_mirror
            for place, k_all, i_all in ((p, k_first, i_first), (pairs + p, k_mirror, i_mirror)):
                k_all, i_all = k_all + neighbour, i_all + neighbour
                kern[pl.ds(place, table_rows, stride=own), :] = k_all
                kern[pl.ds(table_rows * own + place, even_rows, stride=own), :] = i_all[:even_rows]
                kern[pl.ds((table_rows + even_rows) * own + place, 2 * cells, stride=own), :] = -k_all[even_rows:]
        acc[...] = jnp.zeros(acc.shape, F32)

    def gather(layer):
        wait_layer(layer)
        sources = [unpack(layer * plane + p) for p in range(plane)]

        def over(n, inner):
            for p in range(plane):
                i = n * plane + p
                total = add_layer(layer, sources, i)
                for q in range(6):
                    acc[i, q] = total[q]
            return inner

        lax.fori_loop(0, layers, over, 0)

    def finish(layer):
        wait_layer(layer)
        sources = [unpack(layer * plane + p) for p in range(plane)]


        def dispatch(n):
            i = target_back(n)

            @pl.when(i != g)
            def _():
                backward(i).start()

            @pl.when(jnp.logical_and(i == 0, twice))
            def _():
                backward(i, 0).start()

        def serve(n):
            i = target_back(n)
            spread(i, add_layer(layer, sources, i))

        chunk = 3

        def over(n, carry):
            first = 1 + n * chunk
            serve(first)

            @pl.when(n == 0)
            def _():
                dispatch(0)

            @pl.when(n > 0)
            def _():
                for p in range(chunk):
                    dispatch(jnp.maximum(first - chunk + p, 1))

            for p in range(1, chunk):
                serve(first + p)
            return carry

        def spread(i, total):
            for comp in range(3):
                re, im = total[2 * comp], total[2 * comp + 1]
                re_f, im_f = flip(re), flip(im)
                new_re = jnp.where(top, re + re_f, im - im_f)
                new_im = jnp.where(top, im + im_f, re_f - re)
                lone_re = jnp.where(al, re, 2.0 * jnp.where(top, re, -im_f))
                lone_im = jnp.where(al, im, 2.0 * jnp.where(top, re_f, -im))
                new_re = jnp.where(special, lone_re, new_re)
                new_im = jnp.where(special, lone_im, new_im)
                back[i, :, pl.ds(2 * comp * half, half)] = new_re.astype(BF16)
                back[i, :, pl.ds((2 * comp + 1) * half, half)] = new_im.astype(BF16)

        serve(0)
        lax.fori_loop(0, (groups - 1) // chunk, over, 0)
        for p in range(chunk):
            dispatch(groups - chunk + p)

        @pl.when(c == 1)
        def _():
            fields[1, g] = back[g]

    prepare()
    beside = (g > 0).astype(F32) + (g < groups - 1).astype(F32)
    for comp in range(3):
        full = jnp.concatenate([mag[0, comp], mag[1, comp]], axis=0).astype(F32)
        centre = full[:rows]
        total = pltpu.roll(full, 1, 0)[:rows] + pltpu.roll(full, 2 * rows - 1, 0)[:rows]
        total = total + pltpu.roll(centre, 1, 1) + pltpu.roll(centre, 2 * half - 1, 1)
        lap[comp] = EXCHANGE * (total - (4.0 + beside) * centre)

    if late_count:
        @pl.when(lower)
        def _():
            pl.semaphore_wait(hand.at[2], late_count)
            for k in range(1, groups):
                to = target(k)

                @pl.when(is_late(to))
                def _():
                    forward(to).start()

    def step(t, carry):
        gather(group_at(t))
        return carry

    lax.fori_loop(0, layers - 1, step, 0)
    finish(group_at(layers - 1))

    for copy in late[1:]:
        copy.wait()

    def relay(part, n):
        at = pl.ds(n * plane, plane)
        return pltpu.make_async_remote_copy(
            src_ref=fields.at[part, at],
            dst_ref=fields.at[part, at],
            send_sem=rel_sem.at[0],
            recv_sem=rel_sem.at[1],
            device_id=(g, 0),
            device_id_type=MESH,
        )

    own_block = pltpu.make_async_remote_copy(
        src_ref=back.at[g],
        dst_ref=fields.at[0, g],
        send_sem=bwd_send.at[0],
        recv_sem=bwd_recv.at[my_layer],
        device_id=(g, 1),
        device_id_type=MESH,
    )

    @pl.when(c == 0)
    def _():
        own_block.start()

        @pl.when(g == 0)
        def _():
            waiter(fields.at[:, pl.ds(0, groups - plane // 2)], rel_sem.at[0], rel_sem.at[1]).wait_recv()
            at = pl.ds(direct * plane, plane)
            waiter(fields.at[0, at], bwd_send.at[0], bwd_recv.at[direct]).wait_recv()

        @pl.when(g != 0)
        def _():
            waiter(fields, rel_sem.at[0], rel_sem.at[1]).wait_recv()

    @pl.when(c == 1)
    def _():
        for k in range(layers):
            n = relay_at(k)
            for part in (1, 0):
                sem = bwd_recv.at[part * layers + n]
                if part == 1:
                    @pl.when(n == my_layer)
                    def _():
                        waiter(fields.at[1, pl.ds(0, plane - 1)], bwd_send.at[0], sem).wait_recv()

                    @pl.when(n != my_layer)
                    def _():
                        waiter(fields.at[1, pl.ds(0, plane)], bwd_send.at[0], sem).wait_recv()
                else:
                    waiter(fields.at[0, pl.ds(0, plane)], bwd_send.at[0], sem).wait_recv()
                if part == 1:
                    relay(part, n).start()
                else:
                    @pl.when(jnp.logical_or(g != 0, n != direct))
                    def _():
                        relay(part, n).start()

    if whole_tiles:
        modes = fields[...].reshape(2 * groups * own, wide)
    else:
        for part in range(2):
            for i in range(groups):
                stack[pl.ds((part * groups + i) * own, own), :] = fields[part, i].astype(F32)
        modes = stack[...].astype(BF16)
    scale = 1.0 / (2 * rows * 2 * half)
    for comp in range(3):
        at = slice(2 * comp * half, 2 * (comp + 1) * half)
        g_rows = jnp.dot(yi[...], modes[:, at], preferred_element_type=F32).astype(BF16)
        demag = jnp.dot(g_rows, zi[...], preferred_element_type=F32) * scale
        out[comp] = (demag + lap[comp]).astype(BF16)

    waiter(mag.at[0], pair_sem.at[0], swap_recv.at[0]).wait_send()

    @pl.when(c == 0)
    def _():
        own_block.wait_send()

    @pl.when(twice)
    def _():
        backward(0, 0).wait_send()

    @pl.when(c == 1)
    def _():
        @pl.when(g == 0)
        def _():
            waiter(fields.at[:, pl.ds(0, groups - plane // 2)], rel_sem.at[0], rel_sem.at[1]).wait_send()

        @pl.when(g != 0)
        def _():
            waiter(fields, rel_sem.at[0], rel_sem.at[1]).wait_send()

    far(0, pairs).wait_send()
    waiter(back.at[pl.ds(0, groups - 1)], bwd_send.at[0], bwd_recv.at[0]).wait_send()
    waiter(send.at[pl.ds(0, groups - 1)], fwd_send.at[0], fwd_recv.at[0]).wait_send()


def on_device(magnet, newell, *consts):
    rows, _, x_cells, z_total = magnet.shape
    groups = lax.axis_size("gx")
    parts = lax.axis_size("yz")
    assert x_cells == 1 and parts == 2
    y_total = rows * parts
    pairs = y_total // (groups * parts * 2)
    own = 2 * pairs
    half = z_total // 2
    wide = 3 * z_total
    layers = groups // math.gcd(groups, 4)
    any_ref = pl.BlockSpec(memory_space=pl.ANY)
    dma = pltpu.SemaphoreType.DMA
    planes = jnp.transpose(magnet[:, :, 0, :], (1, 0, 2))
    field = pl.pallas_call(
        functools.partial(kernel, groups, pairs),
        out_shape=pltpu.VMEM(planes.shape, BF16),
        in_specs=[any_ref] * 7,
        out_specs=pl.BlockSpec(memory_space=pltpu.VMEM),
        scratch_shapes=[
            pltpu.VMEM((2, 3, rows, z_total), BF16),
            pltpu.VMEM((2, pairs, 6, groups, z_total), BF16),
            pltpu.VMEM((rows, y_total), BF16),
            pltpu.VMEM((rows, y_total), BF16),
            pltpu.VMEM((z_total, z_total), BF16),
            pltpu.VMEM((z_total, z_total), BF16),
            pltpu.VMEM((z_total, half), BF16),
            pltpu.VMEM((y_total, wide), BF16),
            pltpu.VMEM((rows, wide), F32),
            pltpu.VMEM((groups, own, wide), BF16),
            pltpu.VMEM((groups, own, wide), BF16),
            pltpu.VMEM((12 * groups * own, half), F32),
            pltpu.VMEM((groups, 6, own, half), F32),
            pltpu.VMEM((groups, own, wide), BF16),
            pltpu.VMEM((2, groups, own, wide), BF16),
            pltpu.VMEM((y_total, wide), F32),
            pltpu.VMEM((3, rows, z_total), F32),
            dma((6,)),
            dma((1,)),
            dma((1,)),
            dma((3,)),
            dma((1,)),
            dma((layers,)),
            dma((1,)),
            dma((2 * layers,)),
            dma((2,)),
            pltpu.SemaphoreType.REGULAR((3,)),
        ],
        compiler_params=pltpu.CompilerParams(collective_id=0, has_side_effects=True),
    )(planes, newell, *consts)
    return jnp.transpose(field, (1, 0, 2))[:, :, None, :]


def solution(mesh):
    groups, parts = mesh.shape["gx"], mesh.shape["yz"]

    def run(magnet, newell):
        consts = tables(groups, parts, magnet.shape[0], magnet.shape[3])
        body = lambda m, n: on_device(m, n, *[jnp.asarray(t) for t in consts])
        return jax.shard_map(
            body,
            mesh=mesh,
            in_specs=(P("yz", None, "gx", None), P("yz", None, None, None)),
            out_specs=P("yz", None, "gx", None),
            check_vma=False,
        )(magnet, newell)

    return run
```

```python
import functools
import math

import jax
import jax.numpy as jnp
import ml_dtypes
import numpy as np
from jax import lax
from jax.experimental import pallas as pl
from jax.experimental.pallas import tpu as pltpu
from jax.sharding import PartitionSpec as P

EXCHANGE = 0.2
F32 = jnp.float32
BF16 = jnp.bfloat16
MESH = pl.DeviceIdType.MESH


def tables(groups, parts, y_total, z_total):
    pairs = y_total // (groups * parts * 2)
    rows = y_total // parts
    half_y = y_total // 2

    def trig(k, n, length):
        angle = (k[:, None] * n[None, :] % length) * (2.0 * math.pi / length)
        return np.cos(angle), np.sin(angle)

    def y_rows(part, n):
        blocks = []
        for m in range(groups):
            t = (m * parts + part) * pairs + np.arange(pairs)
            cos, sin = trig(t, n, y_total)
            if t[0] == 0:
                sin[0] = trig(np.array([half_y]), n, y_total)[0][0]
            blocks += [cos, sin]
        return np.concatenate(blocks)

    half = z_total // 2
    cos, sin = trig(np.arange(z_total), np.arange(half), z_total)
    alternate = np.cos(math.pi * np.arange(z_total))
    z_fwd = np.concatenate([cos, -sin], axis=1)
    z_fwd[:, half] = alternate
    z_inv = -np.concatenate([cos, -sin], axis=1).T
    z_inv[0] = -0.5
    z_inv[half] = -0.5 * alternate
    reverse = np.zeros((z_total, half))
    for k in range(half):
        reverse[-k % z_total, k] = 1.0
    forward, inverse = [], []
    for part in range(parts):
        own_first = (np.arange(y_total) + part * rows) % y_total
        forward.append(y_rows(part, own_first))
        inverse.append(np.concatenate([y_rows(other, own_first[:rows]) for other in range(parts)]).T)
    cast = lambda a: np.asarray(a, np.float32).astype(ml_dtypes.bfloat16)
    return cast(np.stack(forward)), cast(np.stack(inverse)), cast(z_fwd), cast(z_inv), cast(reverse)


def kernel(
    groups, pairs, magnet, newell, y_fwd, y_inv, z_fwd, z_inv, rev, out,
    mag, nwl, yf, yi, zf, zi, rv, zrow, spec, send, recv, kern, acc, back, fields, stack,
    lap, load_sem, near_sem, swap_recv, pair_sem, fwd_send, fwd_recv, bwd_send, bwd_recv,
    rel_sem, hand,
):
    g = lax.axis_index("gx")
    c = lax.axis_index("yz")
    other = 1 - c
    own = 2 * pairs
    rows = magnet.shape[1]
    cells = groups
    half = magnet.shape[2] // 2
    wide = 6 * half
    plane = math.gcd(groups, 4)
    layers = groups // plane
    whole_tiles = own % 8 == 0

    my_layer = g // plane

    def is_late(b):
        return b // plane + lax.rem(b, plane) // 2 + lax.rem(b, 2) >= layers + 1

    late_count = sum(int(b // plane + b % plane // 2 + b % 2 >= layers + 1) for b in range(groups))
    lower = g < groups // 2
    low = 2 * my_layer < layers
    from_edge = jnp.where(low, my_layer, layers - 1 - my_layer)

    def layer_at(t):
        v = jnp.where(t <= from_edge, from_edge - t, t)
        return jnp.where(low, v, layers - 1 - v)

    def target(k):
        return lax.rem(g + k, groups)

    def target_back(k):
        zero_at = lax.rem(groups - g, groups)
        return jnp.where(k == 0, 0, jnp.where(k <= zero_at, target(jnp.maximum(k - 1, 0)), target(k)))

    def group_at(t):
        return lax.rem(my_layer + layers - t, layers)

    def relay_at(t):
        return jnp.where(jnp.logical_and(my_layer == layers - 1, t >= 2), t - 2, jnp.where(t <= my_layer, my_layer - t, t))

    barrier = pltpu.get_barrier_semaphore()
    loads = [
        pltpu.make_async_copy(magnet.at[comp], mag.at[0, comp], load_sem.at[0]) for comp in range(3)
    ]
    tabs = [
        pltpu.make_async_copy(z_fwd, zf, load_sem.at[1]),
        pltpu.make_async_copy(y_fwd.at[c], yf, load_sem.at[2]),
    ]
    late = [
        pltpu.make_async_copy(rev, rv, load_sem.at[3]),
        pltpu.make_async_copy(y_inv.at[c], yi, load_sem.at[4]),
        pltpu.make_async_copy(z_inv, zi, load_sem.at[5]),
    ]
    for copy in loads:
        copy.start()

    @pl.when(c == 0)
    def _():
        pl.semaphore_signal(barrier, inc=1, device_id=(g, 1), device_id_type=MESH)

    for copy in tabs:
        copy.start()
    for r in range(1, groups):
        to = lax.rem(g + r, groups)

        @pl.when(jnp.logical_or(jnp.logical_not(is_late(g)), to >= groups // 2))
        def _():
            pl.semaphore_signal(barrier, inc=1, device_id=(to, 0), device_id_type=MESH)

    def newell_row(part, p):
        t = (2 * g + part) * pairs + p
        return (1 - c) * t + c * lax.rem(rows - t, rows)

    near = [
        pltpu.make_async_copy(newell.at[newell_row(c, p)], nwl.at[c, p], near_sem.at[0]) for p in range(pairs)
    ]

    def waiter(ref, send_sem, recv_sem):
        return pltpu.make_async_remote_copy(
            src_ref=ref,
            dst_ref=ref,
            send_sem=send_sem,
            recv_sem=recv_sem,
            device_id=(g, other),
            device_id_type=MESH,
        )

    @pl.when(c == 1)
    def _():
        pl.semaphore_wait(barrier, 1)
        pl.semaphore_signal(hand.at[0], inc=1, device_id=(g, 0), device_id_type=MESH)

    @pl.when(c == 0)
    def _():
        pl.semaphore_wait(hand.at[0], 1)

    def meet():
        @pl.when(c == 0)
        def _():
            pl.semaphore_wait(barrier, 2 * (groups - 1 - late_count * lower.astype(jnp.int32)))

            @pl.when(is_late(g))
            def _():
                for to in range(groups // 2):
                    for core in range(2):
                        pl.semaphore_signal(hand.at[2], inc=1, device_id=(to, core), device_id_type=MESH)

            pl.semaphore_signal(hand.at[1], inc=1, device_id=(g, 1), device_id_type=MESH)

        @pl.when(c == 1)
        def _():
            pl.semaphore_wait(hand.at[1], 1)

    @pl.when(is_late(g))
    def _():
        meet()

    swap = [
        pltpu.make_async_remote_copy(
            src_ref=mag.at[0, comp],
            dst_ref=mag.at[1, comp],
            send_sem=pair_sem.at[0],
            recv_sem=swap_recv.at[0],
            device_id=(g, other),
            device_id_type=MESH,
        )
        for comp in range(3)
    ]
    pltpu.make_async_copy(mag.at[0], mag.at[0], load_sem.at[0]).wait()
    for copy in swap:
        copy.start()

    def far(p, count):
        at = pl.ds(p, count)
        row = newell_row(other, p)
        return pltpu.make_async_remote_copy(
            src_ref=newell.at[pl.ds(row, 1)] if count == 1 else nwl.at[c, at],
            dst_ref=nwl.at[c, at],
            send_sem=pair_sem.at[1],
            recv_sem=pair_sem.at[2],
            device_id=(g, other),
            device_id_type=MESH,
        )

    for copy in near + late:
        copy.start()
    for p in range(pairs):
        far(p, 1).start()

    for copy in tabs:
        copy.wait()
    def along_z(side, comp):
        return jnp.dot(mag[side, comp], zf[...], preferred_element_type=F32).astype(BF16)

    for comp in range(3):
        zrow[pl.ds(0, rows), pl.ds(2 * comp * half, 2 * half)] = along_z(0, comp)
    spec[...] = jnp.dot(yf[:, :rows], zrow[pl.ds(0, rows), :], preferred_element_type=F32)
    waiter(mag.at[1], pair_sem.at[0], swap_recv.at[0]).wait_recv()
    for comp in range(3):
        at = pl.ds(2 * comp * half, 2 * half)
        part = spec[:, at] + jnp.dot(yf[:, rows:], along_z(1, comp), preferred_element_type=F32)
        if whole_tiles:
            for i in range(groups):
                send[i, :, at] = part[i * own : (i + 1) * own].astype(BF16)
        else:
            spec[:, at] = part
    if not whole_tiles:
        for i in range(groups):
            send[i] = spec[pl.ds(i * own, own), :].astype(BF16)

    @pl.when(jnp.logical_not(is_late(g)))
    def _():
        meet()

    def forward(to):
        return pltpu.make_async_remote_copy(
            src_ref=send.at[to],
            dst_ref=recv.at[g],
            send_sem=fwd_send.at[0],
            recv_sem=fwd_recv.at[my_layer],
            device_id=(to, c),
            device_id_type=MESH,
        )

    for k in range(1, groups):
        to = target(k)

        @pl.when(jnp.logical_not(jnp.logical_and(lower, is_late(to))))
        def _():
            forward(to).start()

    lane = lax.broadcasted_iota(jnp.int32, (own, half), 1)
    row = lax.broadcasted_iota(jnp.int32, (own, half), 0)
    top = row < pairs

    first_t = (2 * g + c) * pairs + lax.rem(row, pairs)
    al = first_t == 0
    ln = jnp.logical_and(lane == 0, first_t > 0)
    special, ln_low = jnp.logical_or(al, ln), jnp.logical_and(ln, jnp.logical_not(top))

    def flip(v):
        return jnp.concatenate([v[pairs:], v[:pairs]], axis=0)

    def wait_layer(layer):
        sem = fwd_recv.at[layer]

        @pl.when(layer == my_layer)
        def _():
            waiter(recv.at[pl.ds(0, plane - 1)], fwd_send.at[0], sem).wait_recv()

        @pl.when(layer != my_layer)
        def _():
            waiter(recv.at[pl.ds(0, plane)], fwd_send.at[0], sem).wait_recv()

    def unpack(j):
        block = recv[j].astype(F32)
        parts = []
        for comp in range(3):
            re = block[:, 2 * comp * half : (2 * comp + 1) * half]
            im = block[:, (2 * comp + 1) * half : (2 * comp + 2) * half]
            re_f, im_f = flip(re), flip(im)
            new_re = jnp.where(top, re + im_f, re_f - im)
            new_im = jnp.where(top, im - re_f, im_f + re)
            lone_re = jnp.where(ln_low, im_f, re)
            lone_im = jnp.where(al, im, -jnp.where(top, re_f, im))
            parts.append(jnp.where(special, lone_re, new_re))
            parts.append(jnp.where(special, lone_im, new_im))
        return parts

    def k_of(entry, d):
        start = pl.multiple_of((entry * cells + d) * own, own)
        return kern[pl.ds(start, own), :]

    def add_layer(layer, sources, i):
        total = [acc[i, q] for q in range(6)]
        for p in range(plane):
            j = layer * plane + p
            d = jnp.abs(i - j)
            signed = jnp.where(i >= j, 4, 10)
            xx, yy, zz, yz = (k_of(e, d) for e in range(4))
            xy, xz = k_of(signed, d), k_of(signed + 1, d)
            xxi, yyi, zzi, yzi = (k_of(6 + e, d) for e in range(4))
            xr, xi, yr, yim, zr, zim = sources[p]
            total[0] += xx * xr - xy * yim - xz * zim
            total[1] += xxi * xi + xy * yr + xz * zr
            total[2] += yy * yr + yz * zr - xy * xi
            total[3] += yyi * yim + yzi * zim + xy * xr
            total[4] += yz * yr + zz * zr - xz * xi
            total[5] += yzi * yim + zzi * zim + xz * xr
        return total

    def backward(i, core=1):
        return pltpu.make_async_remote_copy(
            src_ref=back.at[i],
            dst_ref=fields.at[c, g],
            send_sem=bwd_send.at[0],
            recv_sem=bwd_recv.at[c * layers + my_layer],
            device_id=(i, core),
            device_id_type=MESH,
        )

    direct = layers - 1
    twice = jnp.logical_and(c == 0, my_layer == direct)

    def prepare():
        recv[g] = send[g]
        for copy in near:
            copy.wait()
        far(0, pairs).wait_recv()
        late[0].wait()
        table_rows = 6 * cells
        even_rows = 4 * cells
        lane0 = lax.broadcasted_iota(jnp.int32, (table_rows, half), 1) == 0
        even = lax.broadcasted_iota(jnp.int32, (table_rows, half), 0) < even_rows
        sign = jnp.where(even, 1.0, -1.0).astype(F32)
        row_of = lax.broadcasted_iota(jnp.int32, (table_rows, half), 0)
        diagonal = functools.reduce(jnp.logical_or, [row_of == entry * cells + 1 for entry in range(3)])
        neighbour = jnp.where(diagonal, -2.0 * EXCHANGE, 0.0).astype(F32)
        for p in range(pairs):
            first = nwl[0, p].reshape(table_rows, 2 * half)
            mirror = nwl[1, p].reshape(table_rows, 2 * half)
            rev_first = jnp.dot(first, rv[...], preferred_element_type=F32)
            rev_mirror = jnp.dot(mirror, rv[...], preferred_element_type=F32)
            lo_first, hi_first = first[:, :half].astype(F32), first[:, half:].astype(F32)
            lo_mirror, hi_mirror = mirror[:, :half].astype(F32), mirror[:, half:].astype(F32)
            if p == 0:
                alone = ((2 * g + c) * pairs == 0).astype(F32)
                paired = 1.0 - alone
                of_first = alone * rev_first + paired * rev_mirror
                of_mirror = alone * rev_mirror + paired * rev_first
            else:
                of_first, of_mirror = rev_mirror, rev_first
            k_first = lo_first + sign * of_first
            k_mirror = lo_mirror + sign * of_mirror
            middle = hi_first + sign * hi_mirror
            if p == 0:
                i_first = jnp.where(lane0, alone * (2.0 * hi_first) + paired * k_first, k_first)
                i_mirror = jnp.where(lane0, alone * (2.0 * hi_mirror) + paired * middle, k_mirror)
                k_mirror = jnp.where(lane0, alone * k_mirror + paired * middle, k_mirror)
            else:
                k_mirror = jnp.where(lane0, middle, k_mirror)
                i_first, i_mirror = k_first, k_mirror
            for place, k_all, i_all in ((p, k_first, i_first), (pairs + p, k_mirror, i_mirror)):
                k_all, i_all = k_all + neighbour, i_all + neighbour
                kern[pl.ds(place, table_rows, stride=own), :] = k_all
                kern[pl.ds(table_rows * own + place, even_rows, stride=own), :] = i_all[:even_rows]
                kern[pl.ds((table_rows + even_rows) * own + place, 2 * cells, stride=own), :] = -k_all[even_rows:]
        acc[...] = jnp.zeros(acc.shape, F32)

    def gather(layer):
        wait_layer(layer)
        sources = [unpack(layer * plane + p) for p in range(plane)]

        def over(n, inner):
            for p in range(plane):
                i = n * plane + p
                total = add_layer(layer, sources, i)
                for q in range(6):
                    acc[i, q] = total[q]
            return inner

        lax.fori_loop(0, layers, over, 0)

    def finish(layer):
        wait_layer(layer)
        sources = [unpack(layer * plane + p) for p in range(plane)]


        def dispatch(n):
            i = target_back(n)

            @pl.when(i != g)
            def _():
                backward(i).start()

            @pl.when(jnp.logical_and(i == 0, twice))
            def _():
                backward(i, 0).start()

        def serve(n):
            i = target_back(n)
            spread(i, add_layer(layer, sources, i))

        chunk = 3

        def over(n, carry):
            first = 1 + n * chunk
            serve(first)

            @pl.when(n == 0)
            def _():
                dispatch(0)

            @pl.when(n > 0)
            def _():
                for p in range(chunk):
                    dispatch(jnp.maximum(first - chunk + p, 1))

            for p in range(1, chunk):
                serve(first + p)
            return carry

        def spread(i, total):
            for comp in range(3):
                re, im = total[2 * comp], total[2 * comp + 1]
                re_f, im_f = flip(re), flip(im)
                new_re = jnp.where(top, re + re_f, im - im_f)
                new_im = jnp.where(top, im + im_f, re_f - re)
                lone_re = jnp.where(al, re, 2.0 * jnp.where(top, re, -im_f))
                lone_im = jnp.where(al, im, 2.0 * jnp.where(top, re_f, -im))
                new_re = jnp.where(special, lone_re, new_re)
                new_im = jnp.where(special, lone_im, new_im)
                back[i, :, pl.ds(2 * comp * half, half)] = new_re.astype(BF16)
                back[i, :, pl.ds((2 * comp + 1) * half, half)] = new_im.astype(BF16)

        serve(0)
        lax.fori_loop(0, (groups - 1) // chunk, over, 0)
        for p in range(chunk):
            dispatch(groups - chunk + p)

        @pl.when(c == 1)
        def _():
            fields[1, g] = back[g]

    prepare()
    beside = (g > 0).astype(F32) + (g < groups - 1).astype(F32)
    for comp in range(3):
        full = jnp.concatenate([mag[0, comp], mag[1, comp]], axis=0).astype(F32)
        centre = full[:rows]
        total = pltpu.roll(full, 1, 0)[:rows] + pltpu.roll(full, 2 * rows - 1, 0)[:rows]
        total = total + pltpu.roll(centre, 1, 1) + pltpu.roll(centre, 2 * half - 1, 1)
        lap[comp] = EXCHANGE * (total - (4.0 + beside) * centre)

    if late_count:
        @pl.when(lower)
        def _():
            pl.semaphore_wait(hand.at[2], late_count)
            for k in range(1, groups):
                to = target(k)

                @pl.when(is_late(to))
                def _():
                    forward(to).start()

    def step(t, carry):
        gather(group_at(t))
        return carry

    lax.fori_loop(0, layers - 1, step, 0)
    finish(group_at(layers - 1))

    for copy in late[1:]:
        copy.wait()

    def relay(part, n):
        at = pl.ds(n * plane, plane)
        return pltpu.make_async_remote_copy(
            src_ref=fields.at[part, at],
            dst_ref=fields.at[part, at],
            send_sem=rel_sem.at[0],
            recv_sem=rel_sem.at[1],
            device_id=(g, 0),
            device_id_type=MESH,
        )

    own_block = pltpu.make_async_remote_copy(
        src_ref=back.at[g],
        dst_ref=fields.at[0, g],
        send_sem=bwd_send.at[0],
        recv_sem=bwd_recv.at[my_layer],
        device_id=(g, 1),
        device_id_type=MESH,
    )

    @pl.when(c == 0)
    def _():
        own_block.start()

        @pl.when(g == 0)
        def _():
            waiter(fields.at[:, pl.ds(0, groups - plane // 2)], rel_sem.at[0], rel_sem.at[1]).wait_recv()
            at = pl.ds(direct * plane, plane)
            waiter(fields.at[0, at], bwd_send.at[0], bwd_recv.at[direct]).wait_recv()

        @pl.when(g != 0)
        def _():
            waiter(fields, rel_sem.at[0], rel_sem.at[1]).wait_recv()

    @pl.when(c == 1)
    def _():
        for part in (1, 0):
            for k in range(layers):
                n = relay_at(k)
                sem = bwd_recv.at[part * layers + n]
                if part == 1:
                    @pl.when(n == my_layer)
                    def _():
                        waiter(fields.at[1, pl.ds(0, plane - 1)], bwd_send.at[0], sem).wait_recv()

                    @pl.when(n != my_layer)
                    def _():
                        waiter(fields.at[1, pl.ds(0, plane)], bwd_send.at[0], sem).wait_recv()
                else:
                    waiter(fields.at[0, pl.ds(0, plane)], bwd_send.at[0], sem).wait_recv()
                if part == 1:
                    relay(part, n).start()
                else:
                    @pl.when(jnp.logical_or(g != 0, n != direct))
                    def _():
                        relay(part, n).start()

    if whole_tiles:
        modes = fields[...].reshape(2 * groups * own, wide)
    else:
        for part in range(2):
            for i in range(groups):
                stack[pl.ds((part * groups + i) * own, own), :] = fields[part, i].astype(F32)
        modes = stack[...].astype(BF16)
    scale = 1.0 / (2 * rows * 2 * half)
    for comp in range(3):
        at = slice(2 * comp * half, 2 * (comp + 1) * half)
        g_rows = jnp.dot(yi[...], modes[:, at], preferred_element_type=F32).astype(BF16)
        demag = jnp.dot(g_rows, zi[...], preferred_element_type=F32) * scale
        out[comp] = (demag + lap[comp]).astype(BF16)

    waiter(mag.at[0], pair_sem.at[0], swap_recv.at[0]).wait_send()

    @pl.when(c == 0)
    def _():
        own_block.wait_send()

    @pl.when(twice)
    def _():
        backward(0, 0).wait_send()

    @pl.when(c == 1)
    def _():
        @pl.when(g == 0)
        def _():
            waiter(fields.at[:, pl.ds(0, groups - plane // 2)], rel_sem.at[0], rel_sem.at[1]).wait_send()

        @pl.when(g != 0)
        def _():
            waiter(fields, rel_sem.at[0], rel_sem.at[1]).wait_send()

    far(0, pairs).wait_send()
    waiter(back.at[pl.ds(0, groups - 1)], bwd_send.at[0], bwd_recv.at[0]).wait_send()
    waiter(send.at[pl.ds(0, groups - 1)], fwd_send.at[0], fwd_recv.at[0]).wait_send()


def on_device(magnet, newell, *consts):
    rows, _, x_cells, z_total = magnet.shape
    groups = lax.axis_size("gx")
    parts = lax.axis_size("yz")
    assert x_cells == 1 and parts == 2
    y_total = rows * parts
    pairs = y_total // (groups * parts * 2)
    own = 2 * pairs
    half = z_total // 2
    wide = 3 * z_total
    layers = groups // math.gcd(groups, 4)
    any_ref = pl.BlockSpec(memory_space=pl.ANY)
    dma = pltpu.SemaphoreType.DMA
    planes = jnp.transpose(magnet[:, :, 0, :], (1, 0, 2))
    field = pl.pallas_call(
        functools.partial(kernel, groups, pairs),
        out_shape=pltpu.VMEM(planes.shape, BF16),
        in_specs=[any_ref] * 7,
        out_specs=pl.BlockSpec(memory_space=pltpu.VMEM),
        scratch_shapes=[
            pltpu.VMEM((2, 3, rows, z_total), BF16),
            pltpu.VMEM((2, pairs, 6, groups, z_total), BF16),
            pltpu.VMEM((rows, y_total), BF16),
            pltpu.VMEM((rows, y_total), BF16),
            pltpu.VMEM((z_total, z_total), BF16),
            pltpu.VMEM((z_total, z_total), BF16),
            pltpu.VMEM((z_total, half), BF16),
            pltpu.VMEM((y_total, wide), BF16),
            pltpu.VMEM((rows, wide), F32),
            pltpu.VMEM((groups, own, wide), BF16),
            pltpu.VMEM((groups, own, wide), BF16),
            pltpu.VMEM((12 * groups * own, half), F32),
            pltpu.VMEM((groups, 6, own, half), F32),
            pltpu.VMEM((groups, own, wide), BF16),
            pltpu.VMEM((2, groups, own, wide), BF16),
            pltpu.VMEM((y_total, wide), F32),
            pltpu.VMEM((3, rows, z_total), F32),
            dma((6,)),
            dma((1,)),
            dma((1,)),
            dma((3,)),
            dma((1,)),
            dma((layers,)),
            dma((1,)),
            dma((2 * layers,)),
            dma((2,)),
            pltpu.SemaphoreType.REGULAR((3,)),
        ],
        compiler_params=pltpu.CompilerParams(collective_id=0, has_side_effects=True),
    )(planes, newell, *consts)
    return jnp.transpose(field, (1, 0, 2))[:, :, None, :]


def solution(mesh):
    groups, parts = mesh.shape["gx"], mesh.shape["yz"]

    def run(magnet, newell):
        consts = tables(groups, parts, magnet.shape[0], magnet.shape[3])
        body = lambda m, n: on_device(m, n, *[jnp.asarray(t) for t in consts])
        return jax.shard_map(
            body,
            mesh=mesh,
            in_specs=(P("yz", None, "gx", None), P("yz", None, None, None)),
            out_specs=P("yz", None, "gx", None),
            check_vma=False,
        )(magnet, newell)

    return run
```

```python
import functools
import math

import jax
import jax.numpy as jnp
import ml_dtypes
import numpy as np
from jax import lax
from jax.experimental import pallas as pl
from jax.experimental.pallas import tpu as pltpu
from jax.sharding import PartitionSpec as P

EXCHANGE = 0.2
F32 = jnp.float32
BF16 = jnp.bfloat16
MESH = pl.DeviceIdType.MESH


def tables(groups, parts, y_total, z_total):
    pairs = y_total // (groups * parts * 2)
    rows = y_total // parts
    half_y = y_total // 2

    def trig(k, n, length):
        angle = (k[:, None] * n[None, :] % length) * (2.0 * math.pi / length)
        return np.cos(angle), np.sin(angle)

    def y_rows(part, n):
        blocks = []
        for m in range(groups):
            t = (m * parts + part) * pairs + np.arange(pairs)
            cos, sin = trig(t, n, y_total)
            if t[0] == 0:
                sin[0] = trig(np.array([half_y]), n, y_total)[0][0]
            blocks += [cos, sin]
        return np.concatenate(blocks)

    half = z_total // 2
    cos, sin = trig(np.arange(z_total), np.arange(half), z_total)
    alternate = np.cos(math.pi * np.arange(z_total))
    z_fwd = np.concatenate([cos, -sin], axis=1)
    z_fwd[:, half] = alternate
    z_inv = -np.concatenate([cos, -sin], axis=1).T
    z_inv[0] = -0.5
    z_inv[half] = -0.5 * alternate
    reverse = np.zeros((z_total, half))
    for k in range(half):
        reverse[-k % z_total, k] = 1.0
    forward, inverse = [], []
    for part in range(parts):
        own_first = (np.arange(y_total) + part * rows) % y_total
        forward.append(y_rows(part, own_first))
        inverse.append(np.concatenate([y_rows(other, own_first[:rows]) for other in range(parts)]).T)
    cast = lambda a: np.asarray(a, np.float32).astype(ml_dtypes.bfloat16)
    return cast(np.stack(forward)), cast(np.stack(inverse)), cast(z_fwd), cast(z_inv), cast(reverse)


def kernel(
    groups, pairs, magnet, newell, y_fwd, y_inv, z_fwd, z_inv, rev, out,
    mag, nwl, yf, yi, zf, zi, rv, zrow, spec, send, recv, kern, acc, back, fields, stack,
    lap, load_sem, near_sem, swap_recv, pair_sem, fwd_send, fwd_recv, bwd_send, bwd_recv,
    rel_sem, hand,
):
    g = lax.axis_index("gx")
    c = lax.axis_index("yz")
    other = 1 - c
    own = 2 * pairs
    rows = magnet.shape[1]
    cells = groups
    half = magnet.shape[2] // 2
    wide = 6 * half
    plane = math.gcd(groups, 4)
    layers = groups // plane
    whole_tiles = own % 8 == 0

    my_layer = g // plane

    def is_late(b):
        return b // plane + lax.rem(b, plane) // 2 + lax.rem(b, 2) >= layers + 1

    late_count = sum(int(b // plane + b % plane // 2 + b % 2 >= layers + 1) for b in range(groups))
    lower = g < groups // 2
    low = 2 * my_layer < layers
    from_edge = jnp.where(low, my_layer, layers - 1 - my_layer)

    def layer_at(t):
        v = jnp.where(t <= from_edge, from_edge - t, t)
        return jnp.where(low, v, layers - 1 - v)

    def target(k):
        return lax.rem(g + k, groups)

    def target_back(k):
        zero_at = lax.rem(groups - g, groups)
        return jnp.where(k == 0, 0, jnp.where(k <= zero_at, target(jnp.maximum(k - 1, 0)), target(k)))

    def group_at(t):
        return lax.rem(my_layer + layers - t, layers)

    def relay_at(t):
        return jnp.where(jnp.logical_and(my_layer == layers - 1, t >= 2), t - 2, jnp.where(t <= my_layer, my_layer - t, t))

    barrier = pltpu.get_barrier_semaphore()
    loads = [
        pltpu.make_async_copy(magnet.at[comp], mag.at[0, comp], load_sem.at[0]) for comp in range(3)
    ]
    tabs = [
        pltpu.make_async_copy(z_fwd, zf, load_sem.at[1]),
        pltpu.make_async_copy(y_fwd.at[c], yf, load_sem.at[1]),
    ]
    late = [
        pltpu.make_async_copy(rev, rv, load_sem.at[2]),
        pltpu.make_async_copy(y_inv.at[c], yi, load_sem.at[3]),
        pltpu.make_async_copy(z_inv, zi, load_sem.at[3]),
    ]
    for copy in loads:
        copy.start()

    @pl.when(c == 0)
    def _():
        pl.semaphore_signal(barrier, inc=1, device_id=(g, 1), device_id_type=MESH)

    for r in range(1, groups):
        to = lax.rem(g + r, groups)

        @pl.when(jnp.logical_or(jnp.logical_not(is_late(g)), to >= groups // 2))
        def _():
            pl.semaphore_signal(barrier, inc=1, device_id=(to, 0), device_id_type=MESH)

    for copy in tabs:
        copy.start()

    def newell_row(part, p):
        t = (2 * g + part) * pairs + p
        return (1 - c) * t + c * lax.rem(rows - t, rows)

    near = [
        pltpu.make_async_copy(newell.at[newell_row(c, p)], nwl.at[c, p], near_sem.at[0]) for p in range(pairs)
    ]

    def waiter(ref, send_sem, recv_sem):
        return pltpu.make_async_remote_copy(
            src_ref=ref,
            dst_ref=ref,
            send_sem=send_sem,
            recv_sem=recv_sem,
            device_id=(g, other),
            device_id_type=MESH,
        )

    @pl.when(c == 1)
    def _():
        pl.semaphore_wait(barrier, 1)
        pl.semaphore_signal(hand.at[0], inc=1, device_id=(g, 0), device_id_type=MESH)

    @pl.when(c == 0)
    def _():
        pl.semaphore_wait(hand.at[0], 1)

    def meet():
        @pl.when(c == 0)
        def _():
            pl.semaphore_wait(barrier, 2 * (groups - 1 - late_count * lower.astype(jnp.int32)))

            @pl.when(is_late(g))
            def _():
                for to in range(groups // 2):
                    for core in range(2):
                        pl.semaphore_signal(hand.at[2], inc=1, device_id=(to, core), device_id_type=MESH)

            pl.semaphore_signal(hand.at[1], inc=1, device_id=(g, 1), device_id_type=MESH)

        @pl.when(c == 1)
        def _():
            pl.semaphore_wait(hand.at[1], 1)

    @pl.when(is_late(g))
    def _():
        meet()

    swap = [
        pltpu.make_async_remote_copy(
            src_ref=mag.at[0, comp],
            dst_ref=mag.at[1, comp],
            send_sem=pair_sem.at[0],
            recv_sem=swap_recv.at[0],
            device_id=(g, other),
            device_id_type=MESH,
        )
        for comp in range(3)
    ]
    pltpu.make_async_copy(mag.at[0], mag.at[0], load_sem.at[0]).wait()
    for copy in swap:
        copy.start()

    def far(p, count):
        at = pl.ds(p, count)
        row = newell_row(other, p)
        return pltpu.make_async_remote_copy(
            src_ref=newell.at[pl.ds(row, 1)] if count == 1 else nwl.at[c, at],
            dst_ref=nwl.at[c, at],
            send_sem=pair_sem.at[1],
            recv_sem=pair_sem.at[2],
            device_id=(g, other),
            device_id_type=MESH,
        )

    for copy in near + late:
        copy.start()
    for p in range(pairs):
        far(p, 1).start()

    pltpu.make_async_copy(mag.at[0], mag.at[0], load_sem.at[1]).wait()
    def along_z(side, comp):
        return jnp.dot(mag[side, comp], zf[...], preferred_element_type=F32).astype(BF16)

    for comp in range(3):
        zrow[pl.ds(0, rows), pl.ds(2 * comp * half, 2 * half)] = along_z(0, comp)
    spec[...] = jnp.dot(yf[:, :rows], zrow[pl.ds(0, rows), :], preferred_element_type=F32)
    waiter(mag.at[1], pair_sem.at[0], swap_recv.at[0]).wait_recv()
    for comp in range(3):
        at = pl.ds(2 * comp * half, 2 * half)
        part = spec[:, at] + jnp.dot(yf[:, rows:], along_z(1, comp), preferred_element_type=F32)
        if whole_tiles:
            for i in range(groups):
                send[i, :, at] = part[i * own : (i + 1) * own].astype(BF16)
        else:
            spec[:, at] = part
    if not whole_tiles:
        for i in range(groups):
            send[i] = spec[pl.ds(i * own, own), :].astype(BF16)

    @pl.when(jnp.logical_not(is_late(g)))
    def _():
        meet()

    def forward(to):
        return pltpu.make_async_remote_copy(
            src_ref=send.at[to],
            dst_ref=recv.at[g],
            send_sem=fwd_send.at[0],
            recv_sem=fwd_recv.at[my_layer],
            device_id=(to, c),
            device_id_type=MESH,
        )

    for k in range(1, groups):
        to = target(k)

        @pl.when(jnp.logical_not(jnp.logical_and(lower, is_late(to))))
        def _():
            forward(to).start()

    lane = lax.broadcasted_iota(jnp.int32, (own, half), 1)
    row = lax.broadcasted_iota(jnp.int32, (own, half), 0)
    top = row < pairs

    first_t = (2 * g + c) * pairs + lax.rem(row, pairs)
    al = first_t == 0
    ln = jnp.logical_and(lane == 0, first_t > 0)
    special, ln_low = jnp.logical_or(al, ln), jnp.logical_and(ln, jnp.logical_not(top))

    def flip(v):
        return jnp.concatenate([v[pairs:], v[:pairs]], axis=0)

    def wait_layer(layer):
        sem = fwd_recv.at[layer]

        @pl.when(layer == my_layer)
        def _():
            waiter(recv.at[pl.ds(0, plane - 1)], fwd_send.at[0], sem).wait_recv()

        @pl.when(layer != my_layer)
        def _():
            waiter(recv.at[pl.ds(0, plane)], fwd_send.at[0], sem).wait_recv()

    def unpack(j):
        block = recv[j].astype(F32)
        parts = []
        for comp in range(3):
            re = block[:, 2 * comp * half : (2 * comp + 1) * half]
            im = block[:, (2 * comp + 1) * half : (2 * comp + 2) * half]
            re_f, im_f = flip(re), flip(im)
            new_re = jnp.where(top, re + im_f, re_f - im)
            new_im = jnp.where(top, im - re_f, im_f + re)
            lone_re = jnp.where(ln_low, im_f, re)
            lone_im = jnp.where(al, im, -jnp.where(top, re_f, im))
            parts.append(jnp.where(special, lone_re, new_re))
            parts.append(jnp.where(special, lone_im, new_im))
        return parts

    def k_of(entry, d):
        start = pl.multiple_of((entry * cells + d) * own, own)
        return kern[pl.ds(start, own), :]

    def add_layer(layer, sources, i):
        total = [acc[i, q] for q in range(6)]
        for p in range(plane):
            j = layer * plane + p
            d = jnp.abs(i - j)
            signed = jnp.where(i >= j, 4, 10)
            xx, yy, zz, yz = (k_of(e, d) for e in range(4))
            xy, xz = k_of(signed, d), k_of(signed + 1, d)
            xxi, yyi, zzi, yzi = (k_of(6 + e, d) for e in range(4))
            xr, xi, yr, yim, zr, zim = sources[p]
            total[0] += xx * xr - xy * yim - xz * zim
            total[1] += xxi * xi + xy * yr + xz * zr
            total[2] += yy * yr + yz * zr - xy * xi
            total[3] += yyi * yim + yzi * zim + xy * xr
            total[4] += yz * yr + zz * zr - xz * xi
            total[5] += yzi * yim + zzi * zim + xz * xr
        return total

    def backward(i, core=1):
        return pltpu.make_async_remote_copy(
            src_ref=back.at[i],
            dst_ref=fields.at[c, g],
            send_sem=bwd_send.at[0],
            recv_sem=bwd_recv.at[c * layers + my_layer],
            device_id=(i, core),
            device_id_type=MESH,
        )

    direct = layers - 1
    twice = jnp.logical_and(c == 0, my_layer == direct)

    def prepare():
        recv[g] = send[g]
        for copy in near:
            copy.wait()
        far(0, pairs).wait_recv()
        late[0].wait()
        table_rows = 6 * cells
        even_rows = 4 * cells
        lane0 = lax.broadcasted_iota(jnp.int32, (table_rows, half), 1) == 0
        even = lax.broadcasted_iota(jnp.int32, (table_rows, half), 0) < even_rows
        sign = jnp.where(even, 1.0, -1.0).astype(F32)
        row_of = lax.broadcasted_iota(jnp.int32, (table_rows, half), 0)
        diagonal = functools.reduce(jnp.logical_or, [row_of == entry * cells + 1 for entry in range(3)])
        neighbour = jnp.where(diagonal, -2.0 * EXCHANGE, 0.0).astype(F32)
        for p in range(pairs):
            first = nwl[0, p].reshape(table_rows, 2 * half)
            mirror = nwl[1, p].reshape(table_rows, 2 * half)
            rev_first = jnp.dot(first, rv[...], preferred_element_type=F32)
            rev_mirror = jnp.dot(mirror, rv[...], preferred_element_type=F32)
            lo_first, hi_first = first[:, :half].astype(F32), first[:, half:].astype(F32)
            lo_mirror, hi_mirror = mirror[:, :half].astype(F32), mirror[:, half:].astype(F32)
            if p == 0:
                alone = ((2 * g + c) * pairs == 0).astype(F32)
                paired = 1.0 - alone
                of_first = alone * rev_first + paired * rev_mirror
                of_mirror = alone * rev_mirror + paired * rev_first
            else:
                of_first, of_mirror = rev_mirror, rev_first
            k_first = lo_first + sign * of_first
            k_mirror = lo_mirror + sign * of_mirror
            middle = hi_first + sign * hi_mirror
            if p == 0:
                i_first = jnp.where(lane0, alone * (2.0 * hi_first) + paired * k_first, k_first)
                i_mirror = jnp.where(lane0, alone * (2.0 * hi_mirror) + paired * middle, k_mirror)
                k_mirror = jnp.where(lane0, alone * k_mirror + paired * middle, k_mirror)
            else:
                k_mirror = jnp.where(lane0, middle, k_mirror)
                i_first, i_mirror = k_first, k_mirror
            for place, k_all, i_all in ((p, k_first, i_first), (pairs + p, k_mirror, i_mirror)):
                k_all, i_all = k_all + neighbour, i_all + neighbour
                kern[pl.ds(place, table_rows, stride=own), :] = k_all
                kern[pl.ds(table_rows * own + place, even_rows, stride=own), :] = i_all[:even_rows]
                kern[pl.ds((table_rows + even_rows) * own + place, 2 * cells, stride=own), :] = -k_all[even_rows:]
        acc[...] = jnp.zeros(acc.shape, F32)

    def gather(layer):
        wait_layer(layer)
        sources = [unpack(layer * plane + p) for p in range(plane)]

        def over(n, inner):
            for p in range(plane):
                i = n * plane + p
                total = add_layer(layer, sources, i)
                for q in range(6):
                    acc[i, q] = total[q]
            return inner

        lax.fori_loop(0, layers, over, 0)

    def finish(layer):
        wait_layer(layer)
        sources = [unpack(layer * plane + p) for p in range(plane)]


        def dispatch(n):
            i = target_back(n)

            @pl.when(i != g)
            def _():
                backward(i).start()

            @pl.when(jnp.logical_and(i == 0, twice))
            def _():
                backward(i, 0).start()

        def serve(n):
            i = target_back(n)
            spread(i, add_layer(layer, sources, i))

        chunk = 3

        def over(n, carry):
            first = 1 + n * chunk
            serve(first)

            @pl.when(n == 0)
            def _():
                dispatch(0)

            @pl.when(n > 0)
            def _():
                for p in range(chunk):
                    dispatch(jnp.maximum(first - chunk + p, 1))

            for p in range(1, chunk):
                serve(first + p)
            return carry

        def spread(i, total):
            for comp in range(3):
                re, im = total[2 * comp], total[2 * comp + 1]
                re_f, im_f = flip(re), flip(im)
                new_re = jnp.where(top, re + re_f, im - im_f)
                new_im = jnp.where(top, im + im_f, re_f - re)
                lone_re = jnp.where(al, re, 2.0 * jnp.where(top, re, -im_f))
                lone_im = jnp.where(al, im, 2.0 * jnp.where(top, re_f, -im))
                new_re = jnp.where(special, lone_re, new_re)
                new_im = jnp.where(special, lone_im, new_im)
                back[i, :, pl.ds(2 * comp * half, half)] = new_re.astype(BF16)
                back[i, :, pl.ds((2 * comp + 1) * half, half)] = new_im.astype(BF16)

        serve(0)
        lax.fori_loop(0, (groups - 1) // chunk, over, 0)
        for p in range(chunk):
            dispatch(groups - chunk + p)

        @pl.when(c == 1)
        def _():
            fields[1, g] = back[g]

    prepare()
    beside = (g > 0).astype(F32) + (g < groups - 1).astype(F32)
    for comp in range(3):
        full = jnp.concatenate([mag[0, comp], mag[1, comp]], axis=0).astype(F32)
        centre = full[:rows]
        total = pltpu.roll(full, 1, 0)[:rows] + pltpu.roll(full, 2 * rows - 1, 0)[:rows]
        total = total + pltpu.roll(centre, 1, 1) + pltpu.roll(centre, 2 * half - 1, 1)
        lap[comp] = EXCHANGE * (total - (4.0 + beside) * centre)

    if late_count:
        @pl.when(lower)
        def _():
            pl.semaphore_wait(hand.at[2], late_count)
            for k in range(1, groups):
                to = target(k)

                @pl.when(is_late(to))
                def _():
                    forward(to).start()

    def step(t, carry):
        gather(group_at(t))
        return carry

    lax.fori_loop(0, layers - 1, step, 0)
    finish(group_at(layers - 1))

    pltpu.make_async_copy(mag.at[0], mag.at[0], load_sem.at[3]).wait()

    def relay(part, n):
        at = pl.ds(n * plane, plane)
        return pltpu.make_async_remote_copy(
            src_ref=fields.at[part, at],
            dst_ref=fields.at[part, at],
            send_sem=rel_sem.at[0],
            recv_sem=rel_sem.at[1],
            device_id=(g, 0),
            device_id_type=MESH,
        )

    own_block = pltpu.make_async_remote_copy(
        src_ref=back.at[g],
        dst_ref=fields.at[0, g],
        send_sem=bwd_send.at[0],
        recv_sem=bwd_recv.at[my_layer],
        device_id=(g, 1),
        device_id_type=MESH,
    )

    @pl.when(c == 0)
    def _():
        own_block.start()

        @pl.when(g == 0)
        def _():
            waiter(fields.at[:, pl.ds(0, groups - plane // 2)], rel_sem.at[0], rel_sem.at[1]).wait_recv()
            at = pl.ds(direct * plane, plane)
            waiter(fields.at[0, at], bwd_send.at[0], bwd_recv.at[direct]).wait_recv()

        @pl.when(g != 0)
        def _():
            waiter(fields, rel_sem.at[0], rel_sem.at[1]).wait_recv()

    @pl.when(c == 1)
    def _():
        for part in (1, 0):
            for k in range(layers):
                n = relay_at(k)
                sem = bwd_recv.at[part * layers + n]
                if part == 1:
                    @pl.when(n == my_layer)
                    def _():
                        waiter(fields.at[1, pl.ds(0, plane - 1)], bwd_send.at[0], sem).wait_recv()

                    @pl.when(n != my_layer)
                    def _():
                        waiter(fields.at[1, pl.ds(0, plane)], bwd_send.at[0], sem).wait_recv()
                else:
                    waiter(fields.at[0, pl.ds(0, plane)], bwd_send.at[0], sem).wait_recv()
                if part == 1:
                    relay(part, n).start()
                else:
                    @pl.when(jnp.logical_or(g != 0, n != direct))
                    def _():
                        relay(part, n).start()

    if whole_tiles:
        modes = fields[...].reshape(2 * groups * own, wide)
    else:
        for part in range(2):
            for i in range(groups):
                stack[pl.ds((part * groups + i) * own, own), :] = fields[part, i].astype(F32)
        modes = stack[...].astype(BF16)
    scale = 1.0 / (2 * rows * 2 * half)
    for comp in range(3):
        at = slice(2 * comp * half, 2 * (comp + 1) * half)
        g_rows = jnp.dot(yi[...], modes[:, at], preferred_element_type=F32).astype(BF16)
        demag = jnp.dot(g_rows, zi[...], preferred_element_type=F32) * scale
        out[comp] = (demag + lap[comp]).astype(BF16)

    waiter(mag.at[0], pair_sem.at[0], swap_recv.at[0]).wait_send()

    @pl.when(c == 0)
    def _():
        own_block.wait_send()

    @pl.when(twice)
    def _():
        backward(0, 0).wait_send()

    @pl.when(c == 1)
    def _():
        @pl.when(g == 0)
        def _():
            waiter(fields.at[:, pl.ds(0, groups - plane // 2)], rel_sem.at[0], rel_sem.at[1]).wait_send()

        @pl.when(g != 0)
        def _():
            waiter(fields, rel_sem.at[0], rel_sem.at[1]).wait_send()

    far(0, pairs).wait_send()
    waiter(back.at[pl.ds(0, groups - 1)], bwd_send.at[0], bwd_recv.at[0]).wait_send()
    waiter(send.at[pl.ds(0, groups - 1)], fwd_send.at[0], fwd_recv.at[0]).wait_send()


def on_device(magnet, newell, *consts):
    rows, _, x_cells, z_total = magnet.shape
    groups = lax.axis_size("gx")
    parts = lax.axis_size("yz")
    assert x_cells == 1 and parts == 2 and rows * parts == z_total
    y_total = rows * parts
    pairs = y_total // (groups * parts * 2)
    own = 2 * pairs
    half = z_total // 2
    wide = 3 * z_total
    layers = groups // math.gcd(groups, 4)
    any_ref = pl.BlockSpec(memory_space=pl.ANY)
    dma = pltpu.SemaphoreType.DMA
    planes = jnp.transpose(magnet[:, :, 0, :], (1, 0, 2))
    field = pl.pallas_call(
        functools.partial(kernel, groups, pairs),
        out_shape=pltpu.VMEM(planes.shape, BF16),
        in_specs=[any_ref] * 7,
        out_specs=pl.BlockSpec(memory_space=pltpu.VMEM),
        scratch_shapes=[
            pltpu.VMEM((2, 3, rows, z_total), BF16),
            pltpu.VMEM((2, pairs, 6, groups, z_total), BF16),
            pltpu.VMEM((rows, y_total), BF16),
            pltpu.VMEM((rows, y_total), BF16),
            pltpu.VMEM((z_total, z_total), BF16),
            pltpu.VMEM((z_total, z_total), BF16),
            pltpu.VMEM((z_total, half), BF16),
            pltpu.VMEM((y_total, wide), BF16),
            pltpu.VMEM((rows, wide), F32),
            pltpu.VMEM((groups, own, wide), BF16),
            pltpu.VMEM((groups, own, wide), BF16),
            pltpu.VMEM((12 * groups * own, half), F32),
            pltpu.VMEM((groups, 6, own, half), F32),
            pltpu.VMEM((groups, own, wide), BF16),
            pltpu.VMEM((2, groups, own, wide), BF16),
            pltpu.VMEM((y_total, wide), F32),
            pltpu.VMEM((3, rows, z_total), F32),
            dma((4,)),
            dma((1,)),
            dma((1,)),
            dma((3,)),
            dma((1,)),
            dma((layers,)),
            dma((1,)),
            dma((2 * layers,)),
            dma((2,)),
            pltpu.SemaphoreType.REGULAR((3,)),
        ],
        compiler_params=pltpu.CompilerParams(collective_id=0, has_side_effects=True),
    )(planes, newell, *consts)
    return jnp.transpose(field, (1, 0, 2))[:, :, None, :]


def solution(mesh):
    groups, parts = mesh.shape["gx"], mesh.shape["yz"]

    def run(magnet, newell):
        consts = tables(groups, parts, magnet.shape[0], magnet.shape[3])
        body = lambda m, n: on_device(m, n, *[jnp.asarray(t) for t in consts])
        return jax.shard_map(
            body,
            mesh=mesh,
            in_specs=(P("yz", None, "gx", None), P("yz", None, None, None)),
            out_specs=P("yz", None, "gx", None),
            check_vma=False,
        )(magnet, newell)

    return run
```
